32 devices in a mesh: band: 16 (over z, y, core), slab: 2 (over x).
Axes of the slice: x: 2, y: 2, z: 4, core: 2. Of those that a mesh axis runs over, the one named last changes fastest.
Arguments:
- orbitals: bfloat16 [32, 32, 4096], P('band', 'slab'), may hold values from -6 to 6
- occupation: bfloat16 [32], P('band'), may hold values from 0.25 to 1
Outputs:
- exchange_field: float32 [32, 32, 4096], P('band', 'slab')
The draws below stay inside these ranges and needn't reach their ends.
All inputs are finite; a program needn't handle non-finite values.
Results may differ from the reference program's by a relative error of at most 0.001.
Values may be sent and summed in bfloat16 or wider, within the bound.
A program may use at most 64 MiB of HBM per device.

```python
import math
import jax
import jax.numpy as jnp
from jax import lax

ORB_DEV = 2
NY = 64
NZ = 64
STEPS = 3
ORBITALS = 32
NX = 32
N_BAND = 16


def levels(own_key, dims, split, least, top_value):
    loudness = 1.0
    for axis_at, shards_of in split:
        steps = jax.random.uniform(jax.random.fold_in(jax.random.fold_in(own_key, 6), axis_at), (shards_of,), jnp.float32, least / len(split), top_value / len(split))
        loudness = loudness * jnp.repeat(jnp.exp(steps), dims[axis_at] // shards_of).reshape((-1,) + (1,) * (len(dims) - 1 - axis_at))
    return loudness


def centred(rng, shape, deviation, limit, shards=(), held_as=jnp.bfloat16):
    array = jax.random.normal(rng, shape, jnp.float32) * deviation
    if len(shards) > 0:
        array = levels(rng, shape, shards, -0.22, 0.18) * array
    return jnp.clip(array, min=-limit, max=limit).astype(held_as)


def setup_inputs(seed: int = 0) -> dict:
    key_list = jax.random.split(jax.random.key(seed), 3)
    return {
        "orbitals": centred(key_list[0], (ORBITALS, NX, NY * NZ), 1.0, 6.0, ((0, 16), (1, 2))),
        "occupation": jnp.clip(jnp.exp(math.log(1.0) - 1.3862944 * jax.random.uniform(key_list[1], (ORBITALS,), jnp.float32) ** levels(key_list[1], (ORBITALS,), ((0, 16),), -0.2, 0.2)), 0.25, 1.0).astype(jnp.bfloat16),
    }


screening = 0.5
ratio_mid = (12.0 + 2.0 * screening) / 12.0
root_term = math.sqrt(ratio_mid * ratio_mid - 1.0)
decay_ratio = ratio_mid - root_term
coeff_zero = 1.0 / (6.0 * root_term)
coeff_one = -2.0 * decay_ratio * coeff_zero
coeff_two = 2.0 * decay_ratio * decay_ratio * coeff_zero

def cross_sum(values):
    rest = ((0, 0),) * (values.ndim - 1)
    padded_y = jnp.pad(values, rest + ((NZ, NZ),))
    along_y = padded_y[..., 2 * NZ:] + padded_y[..., :-2 * NZ]
    narrow = jnp.pad(values, rest + ((1, 1),))
    column = jnp.arange(values.shape[-1], dtype=jnp.int32) % NZ
    left_side = jnp.where(column != 0, narrow[..., :-2], 0.0)
    right_side = jnp.where(column != NZ - 1, narrow[..., 2:], 0.0)
    return along_y + (left_side + right_side)

def neighbour(values):
    padded = jnp.pad(values, ((0, 0), (0, 0), (1, 1), (0, 0)))
    return padded[:, :, 2:] + padded[:, :, :-2] + cross_sum(values)

def reference(orbitals, occupation):
    cells = NY * NZ
    orbital_grid = orbitals.astype(jnp.float32).reshape(N_BAND, ORB_DEV, NX, cells)
    occupied = occupation.astype(jnp.float32).reshape(N_BAND, ORB_DEV)

    def one_block(block_index):
        own_block = lax.dynamic_index_in_dim(orbital_grid, block_index, 0, keepdims=False)
        running = jnp.zeros((ORB_DEV, NX, cells), jnp.float32)
        for visit in range(STEPS + 1):
            source_block = ((block_index - visit) % N_BAND).astype(jnp.int32)
            visitor = lax.dynamic_index_in_dim(orbital_grid, source_block, 0, keepdims=False)
            weights = lax.dynamic_index_in_dim(occupied, source_block, 0, keepdims=False)
            density = own_block[:, None] * visitor[None]
            first_term = -neighbour(density) / 6.0
            second_term = -neighbour(first_term) / 3.0 - density
            potential = coeff_zero * density + coeff_one * first_term + coeff_two * second_term
            running = running - lax.optimization_barrier(jnp.sum(weights[None, :, None, None] * visitor[None] * potential, axis=1))
        return running
    result = lax.map(one_block, jnp.arange(N_BAND, dtype=jnp.int32))
    return result.reshape(ORBITALS, NX, cells)
```

```python
import functools
import math

import jax
import jax.numpy as jnp
from jax import lax
from jax.experimental import pallas as pl
from jax.experimental.pallas import tpu as pltpu
from jax.sharding import PartitionSpec as P

NZ = 64
STEPS = 3
LANES = 128
WIDTH = 2
PAD = 2
TOP = 8
FLAT = ((0, 0), (0, 1), (0, 2), (1, 0), (2, 0), (1, 1), (1, -1))
WIDE = ((0, 1, 0), (0, 2, 0), (0, 1, 1), (0, 1, -1), (1, 1, 0), (1, -1, 0))
MESH = pl.DeviceIdType.MESH


screening = 0.5
ratio_mid = (12.0 + 2.0 * screening) / 12.0
root_term = math.sqrt(ratio_mid * ratio_mid - 1.0)
decay_ratio = ratio_mid - root_term
coeff_zero = 1.0 / (6.0 * root_term)
coeff_one = -2.0 * decay_ratio * coeff_zero
coeff_two = 2.0 * decay_ratio * decay_ratio * coeff_zero

scale = coeff_two / 18.0
inner = -coeff_one / 6.0 / scale
outer = (coeff_zero - coeff_two) / scale


def loop(count, body, unroll=1):
    lax.fori_loop(0, count, lambda i, c: (body(i), c)[1], 0, unroll=unroll)


def lane_tile(t):
    return pl.ds(pl.multiple_of(t * LANES, LANES), LANES)


def kernel(n_band, n_slab, orb_ref, occ_ref, out_ref, slots, edges, halos, own, vis, gram, wide, centre,
           load_sem, send_sem, recv_sem, edge_send, edge_recv):
    orbs, planes, cells = orb_ref.shape
    tiles = cells // LANES
    half = tiles // 2
    mine = STEPS
    band, slab = lax.axis_index("band"), lax.axis_index("slab")
    odd = lax.rem(band, 2)

    def at(by, side=0):
        return {"band": lax.rem(band + by + n_band, n_band), "slab": slab + side}

    sibling = at(1 - 2 * odd)
    has = (slab > 0, slab < n_slab - 1)
    step_of = (-1, 1)
    reach = {mine: 0, 1: 2, 0: 1 + 2 * odd}
    source = {mine: 0, 1: -2, 0: 2 * odd - 3}

    load = pltpu.make_async_copy(orb_ref, slots.at[mine, :, :, :cells], load_sem.at[0])
    load.start()

    barrier = pltpu.get_barrier_semaphore()
    for by in (source[1], source[0]):
        pl.semaphore_signal(barrier, inc=1, device_id=at(by), device_id_type=MESH)
    pl.semaphore_signal(barrier, inc=1, device_id=sibling, device_id_type=MESH)
    for side in range(2):
        @pl.when(has[side])
        def _(side=side):
            for slot in (mine, 1, 0):
                pl.semaphore_signal(barrier, inc=1, device_id=at(source[slot], step_of[side]), device_id_type=MESH)

    lane = lax.broadcasted_iota(jnp.int32, (1, LANES), 1)
    low = lane < NZ
    column = lane % NZ

    def shuffle(a, b):
        turned = pltpu.roll(jnp.where(low, b, a), NZ, 1)
        return jnp.where(low, a, turned), jnp.where(low, turned, b)

    def z_next(value, by):
        return jnp.where(column < NZ - by, pltpu.roll(value, LANES - by, 1), 0.0)

    load.wait()
    for o in range(orbs):
        value = jnp.broadcast_to(occ_ref[:, o:o + 1].astype(jnp.float32), (planes, LANES))
        slots[mine, o, :, cells:] = value.astype(jnp.bfloat16)

    def rows_of(slot, o, k):
        return shuffle(slots[slot, o, :, lane_tile(k)].astype(jnp.float32),
                       slots[slot, o, :, lane_tile(k + half)].astype(jnp.float32))

    def cut(k):
        pairs = [rows_of(mine, o, k) for o in range(orbs)]
        for side in range(2):
            at_plane = 0 if side == 0 else planes - WIDTH
            parts = [pairs[o][h][at_plane:at_plane + WIDTH] for h in range(2) for o in range(orbs)]
            edges[side, k] = jnp.concatenate(parts, axis=0).astype(jnp.bfloat16)

    loop(half, cut, 2)

    for side in range(2):
        @pl.when(jnp.logical_not(has[side]))
        def _(side=side):
            halos[:, side] = jnp.zeros(halos.shape[:1] + halos.shape[2:], jnp.bfloat16)

    sides = has[0].astype(jnp.int32) + has[1].astype(jnp.int32)
    pl.semaphore_wait(barrier, 3 + 3 * sides)

    def edge_copy(side, slot):
        return pltpu.make_async_remote_copy(
            src_ref=edges.at[side], dst_ref=halos.at[slot, 1 - side],
            send_sem=edge_send.at[slot, side], recv_sem=edge_recv.at[slot, 1 - side],
            device_id=at(reach[slot], step_of[side]), device_id_type=MESH)

    def edge_pass(side):
        return pltpu.make_async_remote_copy(
            src_ref=halos.at[1, side], dst_ref=halos.at[2, side],
            send_sem=edge_send.at[2, side], recv_sem=edge_recv.at[2, side],
            device_id=sibling, device_id_type=MESH)

    def edge_wait(side, slot):
        pltpu.make_async_remote_copy(
            src_ref=edges.at[1 - side], dst_ref=halos.at[slot, side],
            send_sem=edge_send.at[slot, 1 - side], recv_sem=edge_recv.at[slot, side],
            device_id=sibling, device_id_type=MESH).wait_recv()

    def block_copy(slot, o):
        return pltpu.make_async_remote_copy(
            src_ref=slots.at[mine, o], dst_ref=slots.at[slot, o], send_sem=send_sem.at[slot, o],
            recv_sem=recv_sem.at[slot, o], device_id=at(reach[slot]), device_id_type=MESH)

    def block_pass(o):
        return pltpu.make_async_remote_copy(
            src_ref=slots.at[1, o], dst_ref=slots.at[2, o], send_sem=send_sem.at[2, o],
            recv_sem=recv_sem.at[2, o], device_id=sibling, device_id_type=MESH)

    def each_side(action):
        for side in range(2):
            pl.when(has[side])(functools.partial(action, side))

    each_side(lambda side: edge_copy(side, mine).start())
    each_side(lambda side: edge_copy(side, 1).start())
    each_side(lambda side: edge_copy(side, 0).start())
    for o in range(orbs):
        block_copy(1, o).start()
        block_copy(0, o).start()

    def prepare(t):
        row = lax.broadcasted_iota(jnp.int32, (planes, LANES), 0)
        lanes = lax.broadcasted_iota(jnp.int32, (planes, LANES), 1)
        col = lanes % NZ
        edge_z = jnp.logical_or(col == 0, col == NZ - 1)
        bottom = jnp.logical_and(t == 0, lanes < NZ)
        top = jnp.logical_and(t == tiles - 1, lanes >= NZ)
        first = jnp.logical_and(row == 0, jnp.logical_not(has[0]))
        last = jnp.logical_and(row == planes - 1, jnp.logical_not(has[1]))
        value = jnp.full((planes, LANES), outer + 6.0, jnp.float32)
        for walled in (edge_z, jnp.logical_or(bottom, top), first, last):
            value = value - jnp.where(walled, 1.0, 0.0)
        centre[t] = value

    loop(tiles, prepare)

    def seam(value, keep_low):
        return jnp.where(low if keep_low else jnp.logical_not(low), pltpu.roll(value, NZ, 1), 0.0)

    def widen(slot, dst):
        def body(k):
            borders = []
            for side in range(2):
                plain = halos[slot, side, k].astype(jnp.float32)
                borders.append((plain, z_next(plain, 1), z_next(plain, 2)))
            for o in range(orbs):
                for h, mid in enumerate(rows_of(slot, o, k)):
                    t = 2 * k + h + PAD
                    r = (h * orbs + o) * WIDTH
                    for which, value in enumerate((mid, z_next(mid, 1), z_next(mid, 2))):
                        dst[o, which, t, TOP:TOP + planes] = value
                        dst[o, which, t, TOP - WIDTH:TOP] = borders[0][which][r:r + WIDTH]
                        dst[o, which, t, TOP + planes:TOP + planes + WIDTH] = borders[1][which][r:r + WIDTH]
        loop(half, body, 2)
        rows = dst.shape[3]
        for o in range(orbs):
            for which in range(2):
                for n in range(PAD):
                    dst[o, which, n] = seam(dst[o, which, tiles + n], False)
                    dst[o, which, tiles + PAD + n] = seam(dst[o, which, PAD + n], True)

    start = TOP - WIDTH
    ext = wide.shape[2]

    def gather(slot, src, fresh):
        weights = [-scale * slots[slot, o, :, cells:].astype(jnp.float32) for o in range(orbs)]
        weights = [jnp.broadcast_to(w[:1], (ext, LANES)) for w in weights]

        def body(t):
            at_t = t + PAD
            w = [weights[o] * src[o, 0, at_t, start:start + ext] for o in range(orbs)]
            for n, (which, dx, dy) in enumerate(WIDE):
                value = None if fresh else wide[n, at_t]
                for o in range(orbs):
                    term = w[o] * src[o, which, at_t + dy, start + dx:start + dx + ext]
                    value = term if value is None else value + term
                wide[n, at_t] = value
            w = [w[o][WIDTH:WIDTH + planes] for o in range(orbs)] if False else [
                weights[o][:planes] * src[o, 0, at_t, TOP:TOP + planes] for o in range(orbs)]
            for n, (which, dy) in enumerate(FLAT):
                value = None if fresh else gram[n, at_t]
                for o in range(orbs):
                    term = w[o] * src[o, which, at_t + dy, TOP:TOP + planes]
                    value = term if value is None else value + term
                gram[n, at_t] = value
        loop(tiles, body, 2)

    def finish(t, i):
        at_t = t + PAD

        def orbital(which, dx=0, dy=0):
            return own[i, which, at_t + dy, TOP + dx:TOP + dx + planes]

        def flat(n, dy=0):
            return gram[n, at_t + dy]

        def deep(n, dx=0, dy=0):
            return wide[n, at_t + dy, WIDTH + dx:WIDTH + dx + planes]

        mid = orbital(0)
        near = orbital(0, 1) * deep(0) + orbital(0, -1) * deep(0, -1)
        near = near + (orbital(0, 0, 1) * flat(1) + orbital(0, 0, -1) * flat(1, -1))
        near = near + orbital(1) * flat(3)
        far = orbital(0, 2) * deep(1) + orbital(0, -2) * deep(1, -2)
        far = far + (orbital(0, 0, 2) * flat(2) + orbital(0, 0, -2) * flat(2, -2))
        far = far + orbital(2) * flat(4)
        diag = orbital(0, 1, 1) * deep(2) + orbital(0, -1, -1) * deep(2, -1, -1)
        diag = diag + (orbital(0, 1, -1) * deep(3) + orbital(0, -1, 1) * deep(3, -1, 1))
        diag = diag + (orbital(1, 1) * deep(4) + orbital(1, -1) * deep(5))
        diag = diag + (orbital(1, 0, 1) * flat(5) + orbital(1, 0, -1) * flat(6))
        back = orbital(0, -1) * deep(4, -1) + orbital(0, 1) * deep(5, 1)
        back = back + (orbital(0, 0, -1) * flat(5, -1) + orbital(0, 0, 1) * flat(6, 1))
        back = inner * (mid * flat(3)) + 2.0 * back
        far = far + pltpu.roll(mid * flat(4), 2, 1) + pltpu.roll(back, 1, 1)
        return centre[t] * (mid * flat(0)) + inner * near + (2.0 * diag + far)

    each_side(lambda side: edge_wait(side, mine))
    widen(mine, own)
    gather(mine, own, True)

    if_odd, if_even = (0, 1, 2), (1, 0, 2)

    def step(k):
        slot = jnp.int32(0)
        for n, (a, b) in enumerate(zip(if_odd, if_even)):
            slot = jnp.where(k == n, jnp.where(odd == 1, a, b), slot)
        for q in range(STEPS):
            @pl.when(slot == q)
            def _(q=q):
                each_side(lambda side: edge_wait(side, q))
                if q == 1:
                    each_side(lambda side: edge_pass(side).start())
                for p in range(orbs):
                    (block_pass(p) if q == 2 else block_copy(q, p)).wait_recv()
                    if q == 1:
                        block_pass(p).start()
        widen(slot, vis)
        gather(slot, vis, False)

    loop(len(if_odd), step)

    for n, (which, dy) in enumerate(FLAT):
        if dy > 0:
            for p in range(dy):
                gram[n, PAD - 1 - p] = seam(gram[n, PAD + tiles - 1 - p], False)
        if dy < 0:
            gram[n, PAD + tiles] = seam(gram[n, PAD], True)
    for n, (which, dx, dy) in enumerate(WIDE):
        if dy > 0:
            wide[n, PAD - 1] = seam(wide[n, PAD + tiles - 1], False)
        if dy < 0:
            wide[n, PAD + tiles] = seam(wide[n, PAD], True)

    def apply(k):
        for i in range(orbs):
            a, b = shuffle(finish(2 * k, i), finish(2 * k + 1, i))
            out_ref[i, :, lane_tile(k)] = a
            out_ref[i, :, lane_tile(k + half)] = b

    loop(half, apply)

    for o in range(orbs):
        block_copy(0, o).wait_send()
        block_copy(1, o).wait_send()
        block_pass(o).wait_send()
    for slot in (mine, 1, 0):
        each_side(lambda side: edge_copy(side, slot).wait_send())
    each_side(lambda side: edge_pass(side).wait_send())


def per_device(n_band, n_slab, orbitals, occupation):
    orbs, planes, cells = orbitals.shape
    tiles = cells // LANES
    ext = -(-(planes + 2 * WIDTH) // 8) * 8
    tall = planes + 2 * TOP
    occ = occupation.reshape(1, orbs)
    f32, bf16 = jnp.float32, jnp.bfloat16
    rows = 2 * orbs * WIDTH
    padded = tiles + 2 * PAD
    return pl.pallas_call(
        functools.partial(kernel, n_band, n_slab),
        out_shape=jax.ShapeDtypeStruct(orbitals.shape, f32),
        in_specs=[pl.BlockSpec(memory_space=pl.ANY), pl.BlockSpec(memory_space=pltpu.VMEM)],
        out_specs=pl.BlockSpec(memory_space=pltpu.VMEM),
        scratch_shapes=[
            pltpu.VMEM((STEPS + 1, orbs, planes, cells + LANES), bf16),
            pltpu.VMEM((2, tiles // 2, rows, LANES), bf16),
            pltpu.VMEM((STEPS + 1, 2, tiles // 2, rows, LANES), bf16),
            pltpu.VMEM((orbs, 3, padded, tall, LANES), f32),
            pltpu.VMEM((orbs, 3, padded, tall, LANES), f32),
            pltpu.VMEM((len(FLAT), padded, planes, LANES), f32),
            pltpu.VMEM((len(WIDE), padded, ext, LANES), f32),
            pltpu.VMEM((tiles, planes, LANES), f32),
            pltpu.SemaphoreType.DMA((1,)),
            pltpu.SemaphoreType.DMA((STEPS, orbs)),
            pltpu.SemaphoreType.DMA((STEPS, orbs)),
            pltpu.SemaphoreType.DMA((STEPS + 1, 2)),
            pltpu.SemaphoreType.DMA((STEPS + 1, 2)),
        ],
        compiler_params=pltpu.CompilerParams(collective_id=0, has_side_effects=True),
        name="exchange",
    )(orbitals, occ)


def solution(mesh):
    in_specs = (P("band", "slab", None), P("band"))
    out_specs = P("band", "slab", None)
    return jax.shard_map(
        functools.partial(per_device, mesh.shape["band"], mesh.shape["slab"]),
        mesh=mesh, in_specs=in_specs, out_specs=out_specs, check_vma=False,
    )
```

```python
import functools
import math

import jax
import jax.numpy as jnp
from jax import lax
from jax.experimental import pallas as pl
from jax.experimental.pallas import tpu as pltpu
from jax.sharding import PartitionSpec as P

NZ = 64
STEPS = 3
LANES = 128
WIDTH = 2
PAD = 2
GROUP = 4
TOP = 8
FLAT = ((0, 0), (0, 1), (0, 2), (1, 0), (2, 0), (1, 1), (1, -1))
WIDE = ((0, 1, 0), (0, 2, 0), (0, 1, 1), (0, 1, -1), (1, 1, 0), (1, -1, 0))
MESH = pl.DeviceIdType.MESH


screening = 0.5
ratio_mid = (12.0 + 2.0 * screening) / 12.0
root_term = math.sqrt(ratio_mid * ratio_mid - 1.0)
decay_ratio = ratio_mid - root_term
coeff_zero = 1.0 / (6.0 * root_term)
coeff_one = -2.0 * decay_ratio * coeff_zero
coeff_two = 2.0 * decay_ratio * decay_ratio * coeff_zero

scale = coeff_two / 18.0
inner = -coeff_one / 6.0 / scale
outer = (coeff_zero - coeff_two) / scale


def loop(count, body, unroll=1):
    lax.fori_loop(0, count, lambda i, c: (body(i), c)[1], 0, unroll=unroll)


def lane_tile(t):
    return pl.ds(pl.multiple_of(t * LANES, LANES), LANES)


def kernel(n_band, n_slab, orb_ref, occ_ref, out_ref, slots, edges, halos, own, vis, gram, wide, centre,
           moves, rest, load_sem, send_sem, recv_sem, edge_send, edge_recv):
    orbs, planes, cells = orb_ref.shape
    tiles = cells // LANES
    half = tiles // 2
    mine = STEPS
    band, slab = lax.axis_index("band"), lax.axis_index("slab")
    odd = lax.rem(band, 2)

    def at(by, side=0):
        return {"band": lax.rem(band + by + n_band, n_band), "slab": slab + side}

    sibling = at(1 - 2 * odd)
    has = (slab > 0, slab < n_slab - 1)
    step_of = (-1, 1)
    reach = {mine: 0, 1: 2, 0: 1 + 2 * odd}
    source = {mine: 0, 1: -2, 0: 2 * odd - 3}

    load = pltpu.make_async_copy(orb_ref, slots.at[mine, :, :, :cells], load_sem.at[0])
    load.start()

    barrier = pltpu.get_barrier_semaphore()
    for by in (source[1], source[0]):
        pl.semaphore_signal(barrier, inc=1, device_id=at(by), device_id_type=MESH)
    pl.semaphore_signal(barrier, inc=1, device_id=sibling, device_id_type=MESH)
    for side in range(2):
        @pl.when(has[side])
        def _(side=side):
            for slot in (mine, 1, 0):
                pl.semaphore_signal(barrier, inc=1, device_id=at(source[slot], step_of[side]), device_id_type=MESH)

    lane = lax.broadcasted_iota(jnp.int32, (1, LANES), 1)
    low = lane < NZ
    column = lane % NZ

    def shuffle(a, b):
        turned = pltpu.roll(jnp.where(low, b, a), NZ, 1)
        return jnp.where(low, a, turned), jnp.where(low, turned, b)

    load.wait()
    for o in range(orbs):
        value = jnp.broadcast_to(occ_ref[:, o:o + 1].astype(jnp.float32), (planes, LANES))
        slots[mine, o, :, cells:] = value.astype(jnp.bfloat16)

    def cut(g):
        parts = ([], [])
        for n in range(GROUP):
            for o in range(orbs):
                pair = [slots[mine, o, :, lane_tile(GROUP * g + n + part * half)].astype(jnp.float32) for part in range(2)]
                for side in range(2):
                    at_plane = 0 if side == 0 else planes - WIDTH
                    parts[side].append(jnp.concatenate([p[at_plane:at_plane + WIDTH] for p in pair], axis=1))
        for side in range(2):
            edges[side, g] = jnp.concatenate(parts[side], axis=0).astype(jnp.bfloat16)

    loop(half // GROUP, cut)

    for side in range(2):
        @pl.when(jnp.logical_not(has[side]))
        def _(side=side):
            halos[:, side] = jnp.zeros(halos.shape[:1] + halos.shape[2:], jnp.bfloat16)

    sides = has[0].astype(jnp.int32) + has[1].astype(jnp.int32)
    pl.semaphore_wait(barrier, 3 + 3 * sides)

    def edge_copy(side, slot):
        return pltpu.make_async_remote_copy(
            src_ref=edges.at[side], dst_ref=halos.at[slot, 1 - side],
            send_sem=edge_send.at[slot, side], recv_sem=edge_recv.at[slot, 1 - side],
            device_id=at(reach[slot], step_of[side]), device_id_type=MESH)

    def edge_pass(side):
        return pltpu.make_async_remote_copy(
            src_ref=halos.at[1, side], dst_ref=halos.at[2, side],
            send_sem=edge_send.at[2, side], recv_sem=edge_recv.at[2, side],
            device_id=sibling, device_id_type=MESH)

    def edge_wait(side, slot):
        pltpu.make_async_remote_copy(
            src_ref=edges.at[1 - side], dst_ref=halos.at[slot, side],
            send_sem=edge_send.at[slot, 1 - side], recv_sem=edge_recv.at[slot, side],
            device_id=sibling, device_id_type=MESH).wait_recv()

    def block_copy(slot, o):
        return pltpu.make_async_remote_copy(
            src_ref=slots.at[mine, o], dst_ref=slots.at[slot, o], send_sem=send_sem.at[slot, o],
            recv_sem=recv_sem.at[slot, o], device_id=at(reach[slot]), device_id_type=MESH)

    def block_pass(o):
        return pltpu.make_async_remote_copy(
            src_ref=slots.at[1, o], dst_ref=slots.at[2, o], send_sem=send_sem.at[2, o],
            recv_sem=recv_sem.at[2, o], device_id=sibling, device_id_type=MESH)

    def each_side(action):
        for side in range(2):
            pl.when(has[side])(functools.partial(action, side))

    each_side(lambda side: edge_copy(side, mine).start())
    each_side(lambda side: edge_copy(side, 1).start())
    each_side(lambda side: edge_copy(side, 0).start())
    for o in range(orbs):
        block_copy(1, o).start()
        block_copy(0, o).start()

    def prepare(t):
        row = lax.broadcasted_iota(jnp.int32, (planes, LANES), 0)
        lanes = lax.broadcasted_iota(jnp.int32, (planes, LANES), 1)
        col = lanes % NZ
        edge_z = jnp.logical_or(col == 0, col == NZ - 1)
        bottom = jnp.logical_and(t == 0, lanes < NZ)
        top = jnp.logical_and(t == tiles - 1, lanes >= NZ)
        first = jnp.logical_and(row == 0, jnp.logical_not(has[0]))
        last = jnp.logical_and(row == planes - 1, jnp.logical_not(has[1]))
        value = jnp.full((planes, LANES), outer + 6.0, jnp.float32)
        for walled in (edge_z, jnp.logical_or(bottom, top), first, last):
            value = value - jnp.where(walled, 1.0, 0.0)
        centre[t] = value

    loop(tiles, prepare)

    source_lane = lax.broadcasted_iota(jnp.int32, (2 * LANES, LANES), 0)
    target_lane = lax.broadcasted_iota(jnp.int32, (2 * LANES, LANES), 1)
    for which in range(3):
        for h in range(2):
            wanted = (target_lane // NZ) * LANES + h * NZ + target_lane % NZ + which
            hit = jnp.logical_and(source_lane == wanted, target_lane % NZ + which < NZ)
            c = (2 * which + h) * LANES
            moves[:, c:c + LANES] = jnp.where(hit, 1.0, 0.0).astype(jnp.bfloat16)

    def seam(value, keep_low):
        return jnp.where(low if keep_low else jnp.logical_not(low), pltpu.roll(value, NZ, 1), 0.0)

    def widen(slot, dst):
        matrix = moves[...]
        for o in range(orbs):
            stacked = jnp.concatenate(
                [jnp.concatenate([slots[slot, o, :, (k + part * half) * LANES:(k + part * half + 1) * LANES]
                                  for part in range(2)], axis=1) for k in range(half)], axis=0)
            moved = jnp.dot(stacked, matrix, preferred_element_type=jnp.float32)
            for k in range(half):
                for n in range(6):
                    dst[o, n // 2, 2 * k + n % 2 + PAD, TOP:TOP + planes] = moved[
                        k * planes:(k + 1) * planes, n * LANES:(n + 1) * LANES]
        for side in range(2):
            stacked = jnp.concatenate([halos[slot, side, g] for g in range(half // GROUP)], axis=0)
            moved = jnp.dot(stacked, matrix[:, :4 * LANES], preferred_element_type=jnp.float32)
            to = TOP - WIDTH if side == 0 else TOP + planes
            for k in range(half):
                for o in range(orbs):
                    r = (k * orbs + o) * WIDTH
                    for n in range(4):
                        dst[o, n // 2, 2 * k + n % 2 + PAD, to:to + WIDTH] = moved[r:r + WIDTH, n * LANES:(n + 1) * LANES]
        for o in range(orbs):
            for which in range(2):
                for n in range(PAD):
                    dst[o, which, n] = seam(dst[o, which, tiles + n], False)
                    dst[o, which, tiles + PAD + n] = seam(dst[o, which, PAD + n], True)

    start = TOP - WIDTH
    ext = wide.shape[2]

    def gather(slot, src, fresh):
        weights = [-scale * slots[slot, o, :, cells:].astype(jnp.float32) for o in range(orbs)]
        weights = [jnp.broadcast_to(w[:1], (ext, LANES)) for w in weights]

        def body(t):
            at_t = t + PAD
            w = [weights[o] * src[o, 0, at_t, start:start + ext] for o in range(orbs)]
            for n, (which, dx, dy) in enumerate(WIDE):
                value = None if fresh else wide[n, at_t]
                for o in range(orbs):
                    term = w[o] * src[o, which, at_t + dy, start + dx:start + dx + ext]
                    value = term if value is None else value + term
                wide[n, at_t] = value
            w = [weights[o][:planes] * src[o, 0, at_t, TOP:TOP + planes] for o in range(orbs)]
            for n, (which, dy) in enumerate(FLAT):
                value = None if fresh else gram[n, at_t]
                for o in range(orbs):
                    term = w[o] * src[o, which, at_t + dy, TOP:TOP + planes]
                    value = term if value is None else value + term
                gram[n, at_t] = value
        loop(tiles, body, 2)

    def finish(t, i):
        at_t = t + PAD

        def orbital(which, dx=0, dy=0):
            return own[i, which, at_t + dy, TOP + dx:TOP + dx + planes]

        def flat(n, dy=0):
            return gram[n, at_t + dy]

        def deep(n, dx=0, dy=0):
            return wide[n, at_t + dy, WIDTH + dx:WIDTH + dx + planes]

        mid = orbital(0)
        near = orbital(0, 1) * deep(0) + orbital(0, -1) * deep(0, -1)
        near = near + (orbital(0, 0, 1) * flat(1) + orbital(0, 0, -1) * flat(1, -1))
        near = near + orbital(1) * flat(3)
        far = orbital(0, 2) * deep(1) + orbital(0, -2) * deep(1, -2)
        far = far + (orbital(0, 0, 2) * flat(2) + orbital(0, 0, -2) * flat(2, -2))
        far = far + orbital(2) * flat(4)
        diag = orbital(0, 1, 1) * deep(2) + orbital(0, -1, -1) * deep(2, -1, -1)
        diag = diag + (orbital(0, 1, -1) * deep(3) + orbital(0, -1, 1) * deep(3, -1, 1))
        diag = diag + (orbital(1, 1) * deep(4) + orbital(1, -1) * deep(5))
        diag = diag + (orbital(1, 0, 1) * flat(5) + orbital(1, 0, -1) * flat(6))
        back = orbital(0, -1) * deep(4, -1) + orbital(0, 1) * deep(5, 1)
        back = back + (orbital(0, 0, -1) * flat(5, -1) + orbital(0, 0, 1) * flat(6, 1))
        back = inner * (mid * flat(3)) + 2.0 * back
        rest[0, i, t] = centre[t] * (mid * flat(0)) + inner * near + (2.0 * diag + far)
        rest[1, i, t] = back
        rest[2, i, t] = mid * flat(4)

    each_side(lambda side: edge_wait(side, mine))
    widen(mine, own)
    gather(mine, own, True)

    if_odd, if_even = (0, 1, 2), (1, 0, 2)

    def step(k):
        slot = jnp.int32(0)
        for n, (a, b) in enumerate(zip(if_odd, if_even)):
            slot = jnp.where(k == n, jnp.where(odd == 1, a, b), slot)
        for q in range(STEPS):
            @pl.when(slot == q)
            def _(q=q):
                each_side(lambda side: edge_wait(side, q))
                if q == 1:
                    each_side(lambda side: edge_pass(side).start())
                for p in range(orbs):
                    (block_pass(p) if q == 2 else block_copy(q, p)).wait_recv()
                    if q == 1:
                        block_pass(p).start()
        widen(slot, vis)
        gather(slot, vis, False)

    loop(len(if_odd), step)

    for n, (which, dy) in enumerate(FLAT):
        if dy > 0:
            for p in range(dy):
                gram[n, PAD - 1 - p] = seam(gram[n, PAD + tiles - 1 - p], False)
        if dy < 0:
            gram[n, PAD + tiles] = seam(gram[n, PAD], True)
    for n, (which, dx, dy) in enumerate(WIDE):
        if dy > 0:
            wide[n, PAD - 1] = seam(wide[n, PAD + tiles - 1], False)
        if dy < 0:
            wide[n, PAD + tiles] = seam(wide[n, PAD], True)

    def products(t):
        for i in range(orbs):
            finish(t, i)

    loop(tiles, products)

    def total(t, i):
        return rest[0, i, t] + pltpu.roll(rest[1, i, t], 1, 1) + pltpu.roll(rest[2, i, t], 2, 1)

    def apply(k):
        for i in range(orbs):
            a, b = shuffle(total(2 * k, i), total(2 * k + 1, i))
            out_ref[i, :, lane_tile(k)] = a
            out_ref[i, :, lane_tile(k + half)] = b

    loop(half, apply, 8)

    for o in range(orbs):
        block_copy(0, o).wait_send()
        block_copy(1, o).wait_send()
        block_pass(o).wait_send()
    for slot in (mine, 1, 0):
        each_side(lambda side: edge_copy(side, slot).wait_send())
    each_side(lambda side: edge_pass(side).wait_send())


def per_device(n_band, n_slab, orbitals, occupation):
    orbs, planes, cells = orbitals.shape
    tiles = cells // LANES
    ext = -(-(planes + 2 * WIDTH) // 8) * 8
    tall = planes + 2 * TOP
    occ = occupation.reshape(1, orbs)
    f32, bf16 = jnp.float32, jnp.bfloat16
    rows, groups = GROUP * orbs * WIDTH, tiles // (2 * GROUP)
    padded = tiles + 2 * PAD
    return pl.pallas_call(
        functools.partial(kernel, n_band, n_slab),
        out_shape=pltpu.VMEM(orbitals.shape, f32),
        in_specs=[pl.BlockSpec(memory_space=pl.ANY), pl.BlockSpec(memory_space=pltpu.VMEM)],
        out_specs=pl.BlockSpec(memory_space=pltpu.VMEM),
        scratch_shapes=[
            pltpu.VMEM((STEPS + 1, orbs, planes, cells + LANES), bf16),
            pltpu.VMEM((2, groups, rows, 2 * LANES), bf16),
            pltpu.VMEM((STEPS + 1, 2, groups, rows, 2 * LANES), bf16),
            pltpu.VMEM((orbs, 3, padded, tall, LANES), f32),
            pltpu.VMEM((orbs, 3, padded, tall, LANES), f32),
            pltpu.VMEM((len(FLAT), padded, planes, LANES), f32),
            pltpu.VMEM((len(WIDE), padded, ext, LANES), f32),
            pltpu.VMEM((tiles, planes, LANES), f32),
            pltpu.VMEM((2 * LANES, 6 * LANES), bf16),
            pltpu.VMEM((3, orbs, tiles, planes, LANES), f32),
            pltpu.SemaphoreType.DMA((1,)),
            pltpu.SemaphoreType.DMA((STEPS, orbs)),
            pltpu.SemaphoreType.DMA((STEPS, orbs)),
            pltpu.SemaphoreType.DMA((STEPS + 1, 2)),
            pltpu.SemaphoreType.DMA((STEPS + 1, 2)),
        ],
        compiler_params=pltpu.CompilerParams(collective_id=0, has_side_effects=True),
        name="exchange",
    )(orbitals, occ)


def solution(mesh):
    in_specs = (P("band", "slab", None), P("band"))
    out_specs = P("band", "slab", None)
    return jax.shard_map(
        functools.partial(per_device, mesh.shape["band"], mesh.shape["slab"]),
        mesh=mesh, in_specs=in_specs, out_specs=out_specs, check_vma=False,
    )
```

```python
import functools
import math

import jax
import jax.numpy as jnp
from jax import lax
from jax.experimental import pallas as pl
from jax.experimental.pallas import tpu as pltpu
from jax.sharding import PartitionSpec as P

NZ = 64
STEPS = 3
LANES = 128
WIDTH = 2
PAD = 2
GROUP = 4
CHUNKS = 4
SENDS = STEPS + 2
TOP = 8
FLAT = ((0, 0), (0, 1), (0, 2), (1, 0), (2, 0), (1, 1), (1, -1))
WIDE = ((0, 1, 0), (0, 2, 0), (0, 1, 1), (0, 1, -1), (1, 1, 0), (1, -1, 0))
MESH = pl.DeviceIdType.MESH


screening = 0.5
ratio_mid = (12.0 + 2.0 * screening) / 12.0
root_term = math.sqrt(ratio_mid * ratio_mid - 1.0)
decay_ratio = ratio_mid - root_term
coeff_zero = 1.0 / (6.0 * root_term)
coeff_one = -2.0 * decay_ratio * coeff_zero
coeff_two = 2.0 * decay_ratio * decay_ratio * coeff_zero

scale = coeff_two / 18.0
inner = -coeff_one / 6.0 / scale
outer = (coeff_zero - coeff_two) / scale


def loop(count, body, unroll=1):
    lax.fori_loop(0, count, lambda i, c: (body(i), c)[1], 0, unroll=unroll)


def lane_tile(t):
    return pl.ds(pl.multiple_of(t * LANES, LANES), LANES)


def kernel(n_band, n_slab, orb_ref, occ_ref, out_ref, slots, edges, halos, own, vis, gram, wide, centre,
           moves, rest, load_sem, send_sem, recv_sem, edge_send, edge_recv):
    orbs, planes, cells = orb_ref.shape
    tiles = cells // LANES
    half = tiles // 2
    groups = half // GROUP
    mine, carry = 0, STEPS + 1
    chunk = half * LANES // CHUNKS
    band, slab = lax.axis_index("band"), lax.axis_index("slab")
    kind = lax.rem(band, 4)
    is_d = kind == 3

    def by_kind(a, b, c, d):
        return jnp.where(kind == 0, a, jnp.where(kind == 1, b, jnp.where(kind == 2, c, d)))

    def at(by, side=0):
        return {"band": lax.rem(band + by + n_band, n_band), "slab": slab + side}

    sibling = at(by_kind(1, -1, 1, -1))
    has = (slab > 0, slab < n_slab - 1)
    step_of = (-1, 1)
    slot_x, reach_x = by_kind(2, 2, 2, carry), by_kind(2, 2, 2, 4)
    slot_y, reach_y = by_kind(1, 3, 1, 1), by_kind(1, 3, 1, 1)
    slot_pass = by_kind(3, 1, 3, 1)

    loads = [pltpu.make_async_copy(orb_ref.at[:, :, part * half * LANES:(part + 1) * half * LANES],
                                   slots.at[mine, :, part], load_sem.at[part]) for part in range(2)]
    for load in loads:
        load.start()

    barrier = pltpu.get_barrier_semaphore()
    sides = has[0].astype(jnp.int32) + has[1].astype(jnp.int32)
    straight = {0: (1, -2, -3), 1: (-1, 2), 2: (-2, 1), 3: (-1, -2, -4)}
    slanted = {0: (-2, -3), 1: (-1,), 2: (-2,), 3: (-1, -2, -4)}

    def greet(by, side=0):
        pl.semaphore_signal(barrier, inc=1, device_id=at(by, side), device_id_type=MESH)

    for which in range(4):
        @pl.when(kind == which)
        def _(which=which):
            for by in sorted(straight[which]):
                greet(by)
            for side in range(2):
                @pl.when(has[side])
                def _(side=side):
                    for by in sorted(slanted[which]) + [0]:
                        greet(by, step_of[side])

    lane = lax.broadcasted_iota(jnp.int32, (1, LANES), 1)
    low = lane < NZ
    column = lane % NZ

    def shuffle(a, b):
        turned = pltpu.roll(jnp.where(low, b, a), NZ, 1)
        return jnp.where(low, a, turned), jnp.where(low, turned, b)

    for load in loads:
        load.wait()
    for side in range(2):
        rows = [jnp.broadcast_to(occ_ref[:, o:o + 1].astype(jnp.float32), (1, 2 * LANES)) for o in range(orbs)]
        rows.append(jnp.zeros((edges.shape[2] - orbs, 2 * LANES), jnp.float32))
        edges[side, groups] = jnp.concatenate(rows, axis=0).astype(jnp.bfloat16)

    def cut(g):
        parts = ([], [])
        for n in range(GROUP):
            for o in range(orbs):
                pair = [slots[mine, o, part, :, lane_tile(GROUP * g + n)].astype(jnp.float32) for part in range(2)]
                for side in range(2):
                    at_plane = 0 if side == 0 else planes - WIDTH
                    parts[side].append(jnp.concatenate([p[at_plane:at_plane + WIDTH] for p in pair], axis=1))
        for side in range(2):
            edges[side, g] = jnp.concatenate(parts[side], axis=0).astype(jnp.bfloat16)

    loop(groups, cut)

    for side in range(2):
        @pl.when(jnp.logical_not(has[side]))
        def _(side=side):
            halos[:, side] = jnp.zeros(halos.shape[:1] + halos.shape[2:], jnp.bfloat16)

    pl.semaphore_wait(barrier, by_kind(2, 3, 2, 3) + sides * by_kind(3, 3, 3, 2))

    def edge_copy(side, slot, by):
        return pltpu.make_async_remote_copy(
            src_ref=edges.at[side], dst_ref=halos.at[slot, 1 - side],
            send_sem=edge_send.at[slot, side], recv_sem=edge_recv.at[slot, 1 - side],
            device_id=at(by, step_of[side]), device_id_type=MESH)

    def edge_pass(side, src, slot, device, sem):
        return pltpu.make_async_remote_copy(
            src_ref=halos.at[src, side], dst_ref=halos.at[slot, side],
            send_sem=edge_send.at[sem, side], recv_sem=edge_recv.at[slot, side],
            device_id=device, device_id_type=MESH)

    def piece(ref, slot, c):
        return ref.at[slot, :, :, :, c * chunk:(c + 1) * chunk]

    def block_copy(src, slot, c, device, sem):
        return pltpu.make_async_remote_copy(
            src_ref=piece(slots, src, c), dst_ref=piece(slots, slot, c), send_sem=send_sem.at[sem, c],
            recv_sem=recv_sem.at[slot, c], device_id=device, device_id_type=MESH)

    def each_side(action):
        for side in range(2):
            pl.when(has[side])(functools.partial(action, side))

    def send_x(c):
        return block_copy(mine, slot_x, c, at(reach_x), 0)

    def send_y(c):
        return block_copy(mine, slot_y, c, at(reach_y), 1)

    def send_on(c):
        return block_copy(2, slot_pass, c, sibling, 2)

    def relays(c):
        return (block_copy(carry, 2, c, at(-2), 3), block_copy(carry, 3, c, at(-1), 4))

    def edge_on(side):
        return edge_pass(side, 2, slot_pass, sibling, SENDS)

    def edge_relays(side):
        return (edge_pass(side, carry, 2, at(-2), SENDS + 1), edge_pass(side, carry, 3, at(-1), SENDS + 2))

    def arrived(slot, c):
        block_copy(mine, slot, c, sibling, 0).wait_recv()

    def edge_arrived(slot):
        each_side(lambda side: edge_pass(side, mine, slot, sibling, 0).wait_recv())

    each_side(lambda side: edge_copy(side, mine, 0).start())
    each_side(lambda side: edge_copy(side, slot_x, reach_x).start())
    pl.when(jnp.logical_not(is_d))(lambda: each_side(lambda side: edge_copy(side, slot_y, reach_y).start()))
    for c in range(CHUNKS):
        send_x(c).start()
        pl.when(jnp.logical_not(is_d))(lambda c=c: send_y(c).start())

    def prepare(t):
        row = lax.broadcasted_iota(jnp.int32, (planes, LANES), 0)
        lanes = lax.broadcasted_iota(jnp.int32, (planes, LANES), 1)
        col = lanes % NZ
        edge_z = jnp.logical_or(col == 0, col == NZ - 1)
        bottom = jnp.logical_and(t == 0, lanes < NZ)
        top = jnp.logical_and(t == tiles - 1, lanes >= NZ)
        first = jnp.logical_and(row == 0, jnp.logical_not(has[0]))
        last = jnp.logical_and(row == planes - 1, jnp.logical_not(has[1]))
        value = jnp.full((planes, LANES), outer + 6.0, jnp.float32)
        for walled in (edge_z, jnp.logical_or(bottom, top), first, last):
            value = value - jnp.where(walled, 1.0, 0.0)
        centre[t] = value

    loop(tiles, prepare)

    source_lane = lax.broadcasted_iota(jnp.int32, (2 * LANES, LANES), 0)
    target_lane = lax.broadcasted_iota(jnp.int32, (2 * LANES, LANES), 1)
    for which in range(3):
        for h in range(2):
            wanted = (target_lane // NZ) * LANES + h * NZ + target_lane % NZ + which
            hit = jnp.logical_and(source_lane == wanted, target_lane % NZ + which < NZ)
            c = (2 * which + h) * LANES
            moves[:, c:c + LANES] = jnp.where(hit, 1.0, 0.0).astype(jnp.bfloat16)

    def seam(value, keep_low):
        return jnp.where(low if keep_low else jnp.logical_not(low), pltpu.roll(value, NZ, 1), 0.0)

    def widen(slot, dst):
        matrix = moves[...]
        for o in range(orbs):
            stacked = jnp.concatenate(
                [jnp.concatenate([slots[slot, o, part, :, k * LANES:(k + 1) * LANES]
                                  for part in range(2)], axis=1) for k in range(half)], axis=0)
            moved = jnp.dot(stacked, matrix, preferred_element_type=jnp.float32)
            for k in range(half):
                for n in range(6):
                    dst[o, n // 2, 2 * k + n % 2 + PAD, TOP:TOP + planes] = moved[
                        k * planes:(k + 1) * planes, n * LANES:(n + 1) * LANES]
        for side in range(2):
            stacked = jnp.concatenate([halos[slot, side, g] for g in range(groups)], axis=0)
            moved = jnp.dot(stacked, matrix[:, :4 * LANES], preferred_element_type=jnp.float32)
            to = TOP - WIDTH if side == 0 else TOP + planes
            for k in range(half):
                for o in range(orbs):
                    r = (k * orbs + o) * WIDTH
                    for n in range(4):
                        dst[o, n // 2, 2 * k + n % 2 + PAD, to:to + WIDTH] = moved[r:r + WIDTH, n * LANES:(n + 1) * LANES]
        for o in range(orbs):
            for which in range(2):
                for n in range(PAD):
                    dst[o, which, n] = seam(dst[o, which, tiles + n], False)
                    dst[o, which, tiles + PAD + n] = seam(dst[o, which, PAD + n], True)

    start = TOP - WIDTH
    ext = wide.shape[2]

    def gather(slot, src, fresh):
        if fresh:
            rows = edges[0, groups]
        else:
            rows = jnp.where(has[0], halos[slot, 0, groups].astype(jnp.float32), halos[slot, 1, groups].astype(jnp.float32))
        rows = -scale * rows[:orbs, :LANES].astype(jnp.float32)
        weights = [jnp.broadcast_to(rows[o:o + 1], (ext, LANES)) for o in range(orbs)]

        def body(t):
            at_t = t + PAD
            w = [weights[o] * src[o, 0, at_t, start:start + ext] for o in range(orbs)]
            for n, (which, dx, dy) in enumerate(WIDE):
                value = None if fresh else wide[n, at_t]
                for o in range(orbs):
                    term = w[o] * src[o, which, at_t + dy, start + dx:start + dx + ext]
                    value = term if value is None else value + term
                wide[n, at_t] = value
            w = [weights[o][:planes] * src[o, 0, at_t, TOP:TOP + planes] for o in range(orbs)]
            for n, (which, dy) in enumerate(FLAT):
                value = None if fresh else gram[n, at_t]
                for o in range(orbs):
                    term = w[o] * src[o, which, at_t + dy, TOP:TOP + planes]
                    value = term if value is None else value + term
                gram[n, at_t] = value
        loop(tiles, body, 2)

    def finish(t, i):
        at_t = t + PAD

        def orbital(which, dx=0, dy=0):
            return own[i, which, at_t + dy, TOP + dx:TOP + dx + planes]

        def flat(n, dy=0):
            return gram[n, at_t + dy]

        def deep(n, dx=0, dy=0):
            return wide[n, at_t + dy, WIDTH + dx:WIDTH + dx + planes]

        mid = orbital(0)
        near = orbital(0, 1) * deep(0) + orbital(0, -1) * deep(0, -1)
        near = near + (orbital(0, 0, 1) * flat(1) + orbital(0, 0, -1) * flat(1, -1))
        near = near + orbital(1) * flat(3)
        far = orbital(0, 2) * deep(1) + orbital(0, -2) * deep(1, -2)
        far = far + (orbital(0, 0, 2) * flat(2) + orbital(0, 0, -2) * flat(2, -2))
        far = far + orbital(2) * flat(4)
        diag = orbital(0, 1, 1) * deep(2) + orbital(0, -1, -1) * deep(2, -1, -1)
        diag = diag + (orbital(0, 1, -1) * deep(3) + orbital(0, -1, 1) * deep(3, -1, 1))
        diag = diag + (orbital(1, 1) * deep(4) + orbital(1, -1) * deep(5))
        diag = diag + (orbital(1, 0, 1) * flat(5) + orbital(1, 0, -1) * flat(6))
        back = orbital(0, -1) * deep(4, -1) + orbital(0, 1) * deep(5, 1)
        back = back + (orbital(0, 0, -1) * flat(5, -1) + orbital(0, 0, 1) * flat(6, 1))
        back = inner * (mid * flat(3)) + 2.0 * back
        rest[0, i, t] = centre[t] * (mid * flat(0)) + inner * near + (2.0 * diag + far)
        rest[1, i, t] = back
        rest[2, i, t] = mid * flat(4)

    edge_arrived(mine)
    widen(mine, own)
    gather(mine, own, True)

    def step(n):
        slot = jnp.where(n == 0, by_kind(3, 1, 2, 1), jnp.where(n == 1, by_kind(2, 2, 1, 2), by_kind(1, 3, 3, 3)))

        @pl.when(slot == 2)
        def _():
            edge_arrived(2)
            each_side(lambda side: edge_on(side).start())

            @pl.when(is_d)
            def _():
                edge_arrived(carry)

                def hand_on(side):
                    for copy in edge_relays(side):
                        copy.start()

                each_side(hand_on)

            for c in range(CHUNKS):
                arrived(2, c)
                send_on(c).start()

                @pl.when(is_d)
                def _(c=c):
                    arrived(carry, c)
                    for copy in relays(c):
                        copy.start()

        @pl.when(slot != 2)
        def _():
            edge_arrived(slot)
            for c in range(CHUNKS):
                arrived(slot, c)

        widen(slot, vis)
        gather(slot, vis, False)

    loop(STEPS, step)

    for n, (which, dy) in enumerate(FLAT):
        if dy > 0:
            for p in range(dy):
                gram[n, PAD - 1 - p] = seam(gram[n, PAD + tiles - 1 - p], False)
        if dy < 0:
            gram[n, PAD + tiles] = seam(gram[n, PAD], True)
    for n, (which, dx, dy) in enumerate(WIDE):
        if dy > 0:
            wide[n, PAD - 1] = seam(wide[n, PAD + tiles - 1], False)
        if dy < 0:
            wide[n, PAD + tiles] = seam(wide[n, PAD], True)

    def products(t):
        for i in range(orbs):
            finish(t, i)

    loop(tiles, products)

    def total(t, i):
        return rest[0, i, t] + pltpu.roll(rest[1, i, t], 1, 1) + pltpu.roll(rest[2, i, t], 2, 1)

    def apply(k):
        for i in range(orbs):
            a, b = shuffle(total(2 * k, i), total(2 * k + 1, i))
            out_ref[i, :, lane_tile(k)] = a
            out_ref[i, :, lane_tile(k + half)] = b

    loop(half, apply, 8)

    each_side(lambda side: edge_copy(side, mine, 0).wait_send())
    each_side(lambda side: edge_copy(side, slot_x, reach_x).wait_send())
    each_side(lambda side: edge_on(side).wait_send())
    for c in range(CHUNKS):
        send_x(c).wait_send()
        send_on(c).wait_send()

    @pl.when(jnp.logical_not(is_d))
    def _():
        each_side(lambda side: edge_copy(side, slot_y, reach_y).wait_send())
        for c in range(CHUNKS):
            send_y(c).wait_send()

    @pl.when(is_d)
    def _():
        def sent(side):
            for copy in edge_relays(side):
                copy.wait_send()

        each_side(sent)
        for c in range(CHUNKS):
            for copy in relays(c):
                copy.wait_send()


def per_device(n_band, n_slab, orbitals, occupation):
    orbs, planes, cells = orbitals.shape
    tiles = cells // LANES
    ext = -(-(planes + 2 * WIDTH) // 8) * 8
    tall = planes + 2 * TOP
    occ = occupation.reshape(1, orbs)
    f32, bf16 = jnp.float32, jnp.bfloat16
    rows, groups = GROUP * orbs * WIDTH, tiles // (2 * GROUP)
    padded = tiles + 2 * PAD
    return pl.pallas_call(
        functools.partial(kernel, n_band, n_slab),
        out_shape=pltpu.VMEM(orbitals.shape, f32),
        in_specs=[pl.BlockSpec(memory_space=pl.ANY), pl.BlockSpec(memory_space=pltpu.VMEM)],
        out_specs=pl.BlockSpec(memory_space=pltpu.VMEM),
        scratch_shapes=[
            pltpu.VMEM((SENDS, orbs, 2, planes, cells // 2), bf16),
            pltpu.VMEM((2, groups + 1, rows, 2 * LANES), bf16),
            pltpu.VMEM((SENDS, 2, groups + 1, rows, 2 * LANES), bf16),
            pltpu.VMEM((orbs, 3, padded, tall, LANES), f32),
            pltpu.VMEM((orbs, 3, padded, tall, LANES), f32),
            pltpu.VMEM((len(FLAT), padded, planes, LANES), f32),
            pltpu.VMEM((len(WIDE), padded, ext, LANES), f32),
            pltpu.VMEM((tiles, planes, LANES), f32),
            pltpu.VMEM((2 * LANES, 6 * LANES), bf16),
            pltpu.VMEM((3, orbs, tiles, planes, LANES), f32),
            pltpu.SemaphoreType.DMA((2,)),
            pltpu.SemaphoreType.DMA((SENDS, CHUNKS)),
            pltpu.SemaphoreType.DMA((SENDS, CHUNKS)),
            pltpu.SemaphoreType.DMA((SENDS + 3, 2)),
            pltpu.SemaphoreType.DMA((SENDS, 2)),
        ],
        compiler_params=pltpu.CompilerParams(collective_id=0, has_side_effects=True),
        name="exchange",
    )(orbitals, occ)


def solution(mesh):
    in_specs = (P("band", "slab", None), P("band"))
    out_specs = P("band", "slab", None)
    return jax.shard_map(
        functools.partial(per_device, mesh.shape["band"], mesh.shape["slab"]),
        mesh=mesh, in_specs=in_specs, out_specs=out_specs, check_vma=False,
    )
```

```python
import functools
import math

import jax
import jax.numpy as jnp
from jax import lax
from jax.experimental import pallas as pl
from jax.experimental.pallas import tpu as pltpu
from jax.sharding import PartitionSpec as P

NZ = 64
STEPS = 3
LANES = 128
WIDTH = 2
PAD = 2
GROUP = 4
CHUNKS = 4
SENDS = STEPS + 1
TOP = 8
FLAT = ((0, 0), (0, 1), (0, 2), (1, 0), (2, 0), (1, 1), (1, -1))
WIDE = ((0, 1, 0), (0, 2, 0), (0, 1, 1), (0, 1, -1), (1, 1, 0), (1, -1, 0))
MESH = pl.DeviceIdType.MESH


screening = 0.5
ratio_mid = (12.0 + 2.0 * screening) / 12.0
root_term = math.sqrt(ratio_mid * ratio_mid - 1.0)
decay_ratio = ratio_mid - root_term
coeff_zero = 1.0 / (6.0 * root_term)
coeff_one = -2.0 * decay_ratio * coeff_zero
coeff_two = 2.0 * decay_ratio * decay_ratio * coeff_zero

scale = coeff_two / 18.0
inner = -coeff_one / 6.0 / scale
outer = (coeff_zero - coeff_two) / scale


def loop(count, body, unroll=1):
    lax.fori_loop(0, count, lambda i, c: (body(i), c)[1], 0, unroll=unroll)


def lane_tile(t):
    return pl.ds(pl.multiple_of(t * LANES, LANES), LANES)


def kernel(n_band, n_slab, orb_ref, occ_ref, out_ref, slots, edges, halos, own, vis, gram, wide, centre,
           moves, rest, occ, load_sem, send_sem, recv_sem, edge_send, edge_recv):
    orbs, planes, cells = orb_ref.shape
    tiles = cells // LANES
    half = tiles // 2
    groups = half // GROUP
    mine = 0
    chunk = half * LANES // CHUNKS
    band, slab = lax.axis_index("band"), lax.axis_index("slab")
    kind = lax.rem(band, 4)
    is_b, is_d = kind == 1, kind == 3

    def by_kind(a, b, c, d):
        return jnp.where(kind == 0, a, jnp.where(kind == 1, b, jnp.where(kind == 2, c, d)))

    def at(by, side=0):
        return {"band": lax.rem(band + by + n_band, n_band), "slab": slab + side}

    sibling = at(by_kind(1, -1, 1, -1))
    has = (slab > 0, slab < n_slab - 1)
    step_of = (-1, 1)
    reach_y, slot_y = by_kind(1, 3, 1, 1), by_kind(1, 3, 1, 1)
    slot_pass = by_kind(3, 1, 3, 1)

    loads = [pltpu.make_async_copy(orb_ref.at[:, :, part * half * LANES:(part + 1) * half * LANES],
                                   slots.at[mine, :, part], load_sem.at[part]) for part in range(2)]
    loads.append(pltpu.make_async_copy(occ_ref, occ, load_sem.at[2]))
    for load in loads:
        load.start()

    barrier = pltpu.get_barrier_semaphore()
    sides = has[0].astype(jnp.int32) + has[1].astype(jnp.int32)
    straight = {0: (1, -2, -3), 1: (-1, -2), 2: (-2, 1, -1), 3: (-1, -2)}
    slanted = {0: (-2, -3), 1: (-1, -2), 2: (-2,), 3: (-1, -2)}

    def greet(by, side=0):
        pl.semaphore_signal(barrier, inc=1, device_id=at(by, side), device_id_type=MESH)

    for which in range(4):
        @pl.when(kind == which)
        def _(which=which):
            for by in sorted(straight[which]):
                greet(by)
            for side in range(2):
                @pl.when(has[side])
                def _(side=side):
                    for by in sorted(slanted[which]) + [0]:
                        greet(by, step_of[side])

    lane = lax.broadcasted_iota(jnp.int32, (1, LANES), 1)
    low = lane < NZ
    column = lane % NZ

    def shuffle(a, b):
        turned = pltpu.roll(jnp.where(low, b, a), NZ, 1)
        return jnp.where(low, a, turned), jnp.where(low, turned, b)

    for load in loads:
        load.wait()
    for side in range(2):
        rows = [jnp.broadcast_to(occ[:, o:o + 1].astype(jnp.float32), (1, 2 * LANES)) for o in range(orbs)]
        rows.append(jnp.zeros((edges.shape[2] - orbs, 2 * LANES), jnp.float32))
        edges[side, groups] = jnp.concatenate(rows, axis=0).astype(jnp.bfloat16)

    def cut(g):
        parts = ([], [])
        for n in range(GROUP):
            for o in range(orbs):
                pair = [slots[mine, o, part, :, lane_tile(GROUP * g + n)].astype(jnp.float32) for part in range(2)]
                for side in range(2):
                    at_plane = 0 if side == 0 else planes - WIDTH
                    parts[side].append(jnp.concatenate([p[at_plane:at_plane + WIDTH] for p in pair], axis=1))
        for side in range(2):
            edges[side, g] = jnp.concatenate(parts[side], axis=0).astype(jnp.bfloat16)

    loop(groups, cut)

    for side in range(2):
        @pl.when(jnp.logical_not(has[side]))
        def _(side=side):
            halos[:, side] = jnp.zeros(halos.shape[:1] + halos.shape[2:], jnp.bfloat16)

    pl.semaphore_wait(barrier, by_kind(2, 4, 2, 2) + sides * by_kind(3, 3, 3, 2))

    def edge_copy(side, slot, by):
        return pltpu.make_async_remote_copy(
            src_ref=edges.at[side], dst_ref=halos.at[slot, 1 - side],
            send_sem=edge_send.at[slot, side], recv_sem=edge_recv.at[slot, 1 - side],
            device_id=at(by, step_of[side]), device_id_type=MESH)

    def edge_pass(side, src, slot, device, sem):
        return pltpu.make_async_remote_copy(
            src_ref=halos.at[src, side], dst_ref=halos.at[slot, side],
            send_sem=edge_send.at[sem, side], recv_sem=edge_recv.at[slot, side],
            device_id=device, device_id_type=MESH)

    def piece(ref, slot, c):
        return ref.at[slot, :, :, :, c * chunk:(c + 1) * chunk]

    def block_copy(src, slot, c, device, sem):
        return pltpu.make_async_remote_copy(
            src_ref=piece(slots, src, c), dst_ref=piece(slots, slot, c), send_sem=send_sem.at[sem, c],
            recv_sem=recv_sem.at[slot, c], device_id=device, device_id_type=MESH)

    def each_side(action):
        for side in range(2):
            pl.when(has[side])(functools.partial(action, side))

    def send_x(c):
        return block_copy(mine, 2, c, at(2), 0)

    def send_y(c):
        return block_copy(mine, slot_y, c, at(reach_y), 1)

    def send_on(c):
        return block_copy(2, slot_pass, c, sibling, 2)

    def relay(c):
        return block_copy(2, 3, c, at(1), 3)

    def edge_on(side):
        return edge_pass(side, 2, slot_pass, sibling, SENDS)

    def edge_relay(side):
        return edge_pass(side, 2, 3, at(1), SENDS + 1)

    def arrived(slot, c):
        block_copy(mine, slot, c, sibling, 0).wait_recv()

    def edge_arrived(slot):
        each_side(lambda side: edge_pass(side, mine, slot, sibling, 0).wait_recv())

    each_side(lambda side: edge_copy(side, mine, 0).start())
    each_side(lambda side: edge_copy(side, 2, 2).start())
    pl.when(jnp.logical_not(is_d))(lambda: each_side(lambda side: edge_copy(side, slot_y, reach_y).start()))
    for c in range(CHUNKS):
        send_x(c).start()
        pl.when(jnp.logical_not(is_d))(lambda c=c: send_y(c).start())

    def prepare(t):
        row = lax.broadcasted_iota(jnp.int32, (planes, LANES), 0)
        lanes = lax.broadcasted_iota(jnp.int32, (planes, LANES), 1)
        col = lanes % NZ
        edge_z = jnp.logical_or(col == 0, col == NZ - 1)
        bottom = jnp.logical_and(t == 0, lanes < NZ)
        top = jnp.logical_and(t == tiles - 1, lanes >= NZ)
        first = jnp.logical_and(row == 0, jnp.logical_not(has[0]))
        last = jnp.logical_and(row == planes - 1, jnp.logical_not(has[1]))
        value = jnp.full((planes, LANES), outer + 6.0, jnp.float32)
        for walled in (edge_z, jnp.logical_or(bottom, top), first, last):
            value = value - jnp.where(walled, 1.0, 0.0)
        centre[t] = value

    loop(tiles, prepare)

    source_lane = lax.broadcasted_iota(jnp.int32, (2 * LANES, LANES), 0)
    target_lane = lax.broadcasted_iota(jnp.int32, (2 * LANES, LANES), 1)
    for which in range(3):
        for h in range(2):
            wanted = (target_lane // NZ) * LANES + h * NZ + target_lane % NZ + which
            hit = jnp.logical_and(source_lane == wanted, target_lane % NZ + which < NZ)
            c = (2 * which + h) * LANES
            moves[:, c:c + LANES] = jnp.where(hit, 1.0, 0.0).astype(jnp.bfloat16)

    def seam(value, keep_low):
        return jnp.where(low if keep_low else jnp.logical_not(low), pltpu.roll(value, NZ, 1), 0.0)

    def widen(slot, dst):
        matrix = moves[...]
        for o in range(orbs):
            stacked = jnp.concatenate(
                [jnp.concatenate([slots[slot, o, part, :, k * LANES:(k + 1) * LANES]
                                  for part in range(2)], axis=1) for k in range(half)], axis=0)
            moved = jnp.dot(stacked, matrix, preferred_element_type=jnp.float32)
            for k in range(half):
                for n in range(6):
                    dst[o, n // 2, 2 * k + n % 2 + PAD, TOP:TOP + planes] = moved[
                        k * planes:(k + 1) * planes, n * LANES:(n + 1) * LANES]
        for side in range(2):
            stacked = jnp.concatenate([halos[slot, side, g] for g in range(groups)], axis=0)
            moved = jnp.dot(stacked, matrix[:, :4 * LANES], preferred_element_type=jnp.float32)
            to = TOP - WIDTH if side == 0 else TOP + planes
            for k in range(half):
                for o in range(orbs):
                    r = (k * orbs + o) * WIDTH
                    for n in range(4):
                        dst[o, n // 2, 2 * k + n % 2 + PAD, to:to + WIDTH] = moved[r:r + WIDTH, n * LANES:(n + 1) * LANES]
        for o in range(orbs):
            for which in range(2):
                for n in range(PAD):
                    dst[o, which, n] = seam(dst[o, which, tiles + n], False)
                    dst[o, which, tiles + PAD + n] = seam(dst[o, which, PAD + n], True)

    start = TOP - WIDTH
    ext = wide.shape[2]

    def gather(slot, src, fresh):
        if fresh:
            rows = edges[0, groups]
        else:
            rows = jnp.where(has[0], halos[slot, 0, groups].astype(jnp.float32), halos[slot, 1, groups].astype(jnp.float32))
        rows = -scale * rows[:orbs, :LANES].astype(jnp.float32)
        weights = [jnp.broadcast_to(rows[o:o + 1], (ext, LANES)) for o in range(orbs)]

        def body(t):
            at_t = t + PAD
            w = [weights[o] * src[o, 0, at_t, start:start + ext] for o in range(orbs)]
            for n, (which, dx, dy) in enumerate(WIDE):
                value = None if fresh else wide[n, at_t]
                for o in range(orbs):
                    term = w[o] * src[o, which, at_t + dy, start + dx:start + dx + ext]
                    value = term if value is None else value + term
                wide[n, at_t] = value
            w = [weights[o][:planes] * src[o, 0, at_t, TOP:TOP + planes] for o in range(orbs)]
            for n, (which, dy) in enumerate(FLAT):
                value = None if fresh else gram[n, at_t]
                for o in range(orbs):
                    term = w[o] * src[o, which, at_t + dy, TOP:TOP + planes]
                    value = term if value is None else value + term
                gram[n, at_t] = value
        loop(tiles, body, 2)

    def finish(t, i):
        at_t = t + PAD

        def orbital(which, dx=0, dy=0):
            return own[i, which, at_t + dy, TOP + dx:TOP + dx + planes]

        def flat(n, dy=0):
            return gram[n, at_t + dy]

        def deep(n, dx=0, dy=0):
            return wide[n, at_t + dy, WIDTH + dx:WIDTH + dx + planes]

        mid = orbital(0)
        near = orbital(0, 1) * deep(0) + orbital(0, -1) * deep(0, -1)
        near = near + (orbital(0, 0, 1) * flat(1) + orbital(0, 0, -1) * flat(1, -1))
        near = near + orbital(1) * flat(3)
        far = orbital(0, 2) * deep(1) + orbital(0, -2) * deep(1, -2)
        far = far + (orbital(0, 0, 2) * flat(2) + orbital(0, 0, -2) * flat(2, -2))
        far = far + orbital(2) * flat(4)
        diag = orbital(0, 1, 1) * deep(2) + orbital(0, -1, -1) * deep(2, -1, -1)
        diag = diag + (orbital(0, 1, -1) * deep(3) + orbital(0, -1, 1) * deep(3, -1, 1))
        diag = diag + (orbital(1, 1) * deep(4) + orbital(1, -1) * deep(5))
        diag = diag + (orbital(1, 0, 1) * flat(5) + orbital(1, 0, -1) * flat(6))
        back = orbital(0, -1) * deep(4, -1) + orbital(0, 1) * deep(5, 1)
        back = back + (orbital(0, 0, -1) * flat(5, -1) + orbital(0, 0, 1) * flat(6, 1))
        back = inner * (mid * flat(3)) + 2.0 * back
        rest[0, i, t] = centre[t] * (mid * flat(0)) + inner * near + (2.0 * diag + far)
        rest[1, i, t] = back
        rest[2, i, t] = mid * flat(4)

    edge_arrived(mine)
    widen(mine, own)
    gather(mine, own, True)

    def step(n):
        slot = jnp.where(n == 0, by_kind(3, 1, 2, 1), jnp.where(n == 1, by_kind(2, 2, 1, 2), by_kind(1, 3, 3, 3)))

        @pl.when(slot == 2)
        def _():
            edge_arrived(2)
            each_side(lambda side: edge_on(side).start())

            pl.when(is_b)(lambda: each_side(lambda side: edge_relay(side).start()))
            for c in range(CHUNKS):
                arrived(2, c)
                send_on(c).start()
                pl.when(is_b)(lambda c=c: relay(c).start())

        @pl.when(slot != 2)
        def _():
            edge_arrived(slot)
            for c in range(CHUNKS):
                arrived(slot, c)

        widen(slot, vis)
        gather(slot, vis, False)

    loop(STEPS, step)

    for n, (which, dy) in enumerate(FLAT):
        if dy > 0:
            for p in range(dy):
                gram[n, PAD - 1 - p] = seam(gram[n, PAD + tiles - 1 - p], False)
        if dy < 0:
            gram[n, PAD + tiles] = seam(gram[n, PAD], True)
    for n, (which, dx, dy) in enumerate(WIDE):
        if dy > 0:
            wide[n, PAD - 1] = seam(wide[n, PAD + tiles - 1], False)
        if dy < 0:
            wide[n, PAD + tiles] = seam(wide[n, PAD], True)

    def products(t):
        for i in range(orbs):
            finish(t, i)

    loop(tiles, products)

    def total(t, i):
        return rest[0, i, t] + pltpu.roll(rest[1, i, t], 1, 1) + pltpu.roll(rest[2, i, t], 2, 1)

    def apply(k):
        for i in range(orbs):
            a, b = shuffle(total(2 * k, i), total(2 * k + 1, i))
            out_ref[i, :, lane_tile(k)] = a
            out_ref[i, :, lane_tile(k + half)] = b

    loop(half, apply, 8)

    each_side(lambda side: edge_copy(side, mine, 0).wait_send())
    each_side(lambda side: edge_copy(side, 2, 2).wait_send())
    each_side(lambda side: edge_on(side).wait_send())
    for c in range(CHUNKS):
        send_x(c).wait_send()
        send_on(c).wait_send()

    @pl.when(jnp.logical_not(is_d))
    def _():
        each_side(lambda side: edge_copy(side, slot_y, reach_y).wait_send())
        for c in range(CHUNKS):
            send_y(c).wait_send()

    @pl.when(is_b)
    def _():
        each_side(lambda side: edge_relay(side).wait_send())
        for c in range(CHUNKS):
            relay(c).wait_send()


def per_device(n_band, n_slab, orbitals, occupation):
    orbs, planes, cells = orbitals.shape
    tiles = cells // LANES
    ext = -(-(planes + 2 * WIDTH) // 8) * 8
    tall = planes + 2 * TOP
    occ = occupation.reshape(1, orbs)
    f32, bf16 = jnp.float32, jnp.bfloat16
    rows, groups = GROUP * orbs * WIDTH, tiles // (2 * GROUP)
    padded = tiles + 2 * PAD
    return pl.pallas_call(
        functools.partial(kernel, n_band, n_slab),
        out_shape=pltpu.VMEM(orbitals.shape, f32),
        in_specs=[pl.BlockSpec(memory_space=pl.ANY)] * 2,
        out_specs=pl.BlockSpec(memory_space=pltpu.VMEM),
        scratch_shapes=[
            pltpu.VMEM((SENDS, orbs, 2, planes, cells // 2), bf16),
            pltpu.VMEM((2, groups + 1, rows, 2 * LANES), bf16),
            pltpu.VMEM((SENDS, 2, groups + 1, rows, 2 * LANES), bf16),
            pltpu.VMEM((orbs, 3, padded, tall, LANES), f32),
            pltpu.VMEM((orbs, 3, padded, tall, LANES), f32),
            pltpu.VMEM((len(FLAT), padded, planes, LANES), f32),
            pltpu.VMEM((len(WIDE), padded, ext, LANES), f32),
            pltpu.VMEM((tiles, planes, LANES), f32),
            pltpu.VMEM((2 * LANES, 6 * LANES), bf16),
            pltpu.VMEM((3, orbs, tiles, planes, LANES), f32),
            pltpu.VMEM(occ.shape, bf16),
            pltpu.SemaphoreType.DMA((3,)),
            pltpu.SemaphoreType.DMA((SENDS, CHUNKS)),
            pltpu.SemaphoreType.DMA((SENDS, CHUNKS)),
            pltpu.SemaphoreType.DMA((SENDS + 2, 2)),
            pltpu.SemaphoreType.DMA((SENDS, 2)),
        ],
        compiler_params=pltpu.CompilerParams(collective_id=0, has_side_effects=True),
        name="exchange",
    )(orbitals, occ)


def solution(mesh):
    in_specs = (P("band", "slab", None), P("band"))
    out_specs = P("band", "slab", None)
    return jax.shard_map(
        functools.partial(per_device, mesh.shape["band"], mesh.shape["slab"]),
        mesh=mesh, in_specs=in_specs, out_specs=out_specs, check_vma=False,
    )
```

```python
import functools
import math

import jax
import jax.numpy as jnp
from jax import lax
from jax.experimental import pallas as pl
from jax.experimental.pallas import tpu as pltpu
from jax.sharding import PartitionSpec as P

NZ = 64
STEPS = 3
LANES = 128
WIDTH = 2
PAD = 2
GROUP = 4
CHUNKS = 4
SENDS = STEPS + 1
TOP = 8
FLAT = ((0, 0), (0, 1), (0, 2), (1, 0), (2, 0), (1, 1), (1, -1))
WIDE = ((0, 1, 0), (0, 2, 0), (0, 1, 1), (0, 1, -1), (1, 1, 0), (1, -1, 0))
MESH = pl.DeviceIdType.MESH


screening = 0.5
ratio_mid = (12.0 + 2.0 * screening) / 12.0
root_term = math.sqrt(ratio_mid * ratio_mid - 1.0)
decay_ratio = ratio_mid - root_term
coeff_zero = 1.0 / (6.0 * root_term)
coeff_one = -2.0 * decay_ratio * coeff_zero
coeff_two = 2.0 * decay_ratio * decay_ratio * coeff_zero

scale = coeff_two / 18.0
inner = -coeff_one / 6.0 / scale
outer = (coeff_zero - coeff_two) / scale


def loop(count, body, unroll=1, start=0):
    lax.fori_loop(start, start + count, lambda i, c: (body(i), c)[1], 0, unroll=unroll)


def lane_tile(t):
    return pl.ds(pl.multiple_of(t * LANES, LANES), LANES)


def kernel(n_band, n_slab, orb_ref, occ_ref, out_ref, slots, edges, halos, own, vis, gram, wide, centre,
           moves, rest, occ, load_sem, send_sem, recv_sem, edge_send, edge_recv):
    orbs, planes, cells = orb_ref.shape
    tiles = cells // LANES
    half = tiles // 2
    groups = half // GROUP
    mine = 0
    chunk = half * LANES // CHUNKS
    band, slab = lax.axis_index("band"), lax.axis_index("slab")
    kind = lax.rem(band, 4)
    is_b, is_d = kind == 1, kind == 3

    def by_kind(a, b, c, d):
        return jnp.where(kind == 0, a, jnp.where(kind == 1, b, jnp.where(kind == 2, c, d)))

    def at(by, side=0):
        return {"band": lax.rem(band + by + n_band, n_band), "slab": slab + side}

    sibling = at(by_kind(1, -1, 1, -1))
    has = (slab > 0, slab < n_slab - 1)
    step_of = (-1, 1)
    reach_y, slot_y = by_kind(1, 3, 1, 1), by_kind(1, 3, 1, 1)
    slot_pass = by_kind(3, 1, 3, 1)

    loads = [pltpu.make_async_copy(orb_ref.at[:, :, part * half * LANES:(part + 1) * half * LANES],
                                   slots.at[mine, :, part], load_sem.at[part]) for part in range(2)]
    loads.append(pltpu.make_async_copy(occ_ref, occ, load_sem.at[2]))
    for load in loads:
        load.start()

    barrier = pltpu.get_barrier_semaphore()
    sides = has[0].astype(jnp.int32) + has[1].astype(jnp.int32)
    straight = {0: (1, -2, -3), 1: (-1, -2), 2: (-2, 1, -1), 3: (-1, -2)}
    slanted = {0: (-2, -3), 1: (-1, -2), 2: (-2,), 3: (-1, -2)}

    def greet(by, side=0):
        pl.semaphore_signal(barrier, inc=1, device_id=at(by, side), device_id_type=MESH)

    for which in range(4):
        @pl.when(kind == which)
        def _(which=which):
            for by in sorted(straight[which]):
                greet(by)
            for side in range(2):
                @pl.when(has[side])
                def _(side=side):
                    for by in sorted(slanted[which]) + [0]:
                        greet(by, step_of[side])

    lane = lax.broadcasted_iota(jnp.int32, (1, LANES), 1)
    low = lane < NZ
    column = lane % NZ

    def shuffle(a, b):
        turned = pltpu.roll(jnp.where(low, b, a), NZ, 1)
        return jnp.where(low, a, turned), jnp.where(low, turned, b)

    for load in loads:
        load.wait()
    for side in range(2):
        rows = [jnp.broadcast_to(occ[:, o:o + 1].astype(jnp.float32), (1, 2 * LANES)) for o in range(orbs)]
        rows.append(jnp.zeros((edges.shape[2] - orbs, 2 * LANES), jnp.float32))
        edges[side, groups] = jnp.concatenate(rows, axis=0).astype(jnp.bfloat16)

    def cut(g):
        parts = ([], [])
        for n in range(GROUP):
            for o in range(orbs):
                pair = [slots[mine, o, part, :, lane_tile(GROUP * g + n)].astype(jnp.float32) for part in range(2)]
                for side in range(2):
                    at_plane = 0 if side == 0 else planes - WIDTH
                    parts[side].append(jnp.concatenate([p[at_plane:at_plane + WIDTH] for p in pair], axis=1))
        for side in range(2):
            edges[side, g] = jnp.concatenate(parts[side], axis=0).astype(jnp.bfloat16)

    loop(groups, cut)

    for side in range(2):
        @pl.when(jnp.logical_not(has[side]))
        def _(side=side):
            halos[:, side] = jnp.zeros(halos.shape[:1] + halos.shape[2:], jnp.bfloat16)

    pl.semaphore_wait(barrier, by_kind(2, 4, 2, 2) + sides * by_kind(3, 3, 3, 2))

    def edge_copy(side, slot, by):
        return pltpu.make_async_remote_copy(
            src_ref=edges.at[side], dst_ref=halos.at[slot, 1 - side],
            send_sem=edge_send.at[slot, side], recv_sem=edge_recv.at[slot, 1 - side],
            device_id=at(by, step_of[side]), device_id_type=MESH)

    def edge_pass(side, src, slot, device, sem):
        return pltpu.make_async_remote_copy(
            src_ref=halos.at[src, side], dst_ref=halos.at[slot, side],
            send_sem=edge_send.at[sem, side], recv_sem=edge_recv.at[slot, side],
            device_id=device, device_id_type=MESH)

    def piece(ref, slot, c):
        return ref.at[slot, :, :, :, c * chunk:(c + 1) * chunk]

    def block_copy(src, slot, c, device, sem):
        return pltpu.make_async_remote_copy(
            src_ref=piece(slots, src, c), dst_ref=piece(slots, slot, c), send_sem=send_sem.at[sem, c],
            recv_sem=recv_sem.at[slot, c], device_id=device, device_id_type=MESH)

    def each_side(action):
        for side in range(2):
            pl.when(has[side])(functools.partial(action, side))

    def send_x(c):
        return block_copy(mine, 2, c, at(2), 0)

    def send_y(c):
        return block_copy(mine, slot_y, c, at(reach_y), 1)

    def send_on(c):
        return block_copy(2, slot_pass, c, sibling, 2)

    def relay(c):
        return block_copy(2, 3, c, at(1), 3)

    def edge_on(side):
        return edge_pass(side, 2, slot_pass, sibling, SENDS)

    def edge_relay(side):
        return edge_pass(side, 2, 3, at(1), SENDS + 1)

    def arrived(slot, c):
        block_copy(mine, slot, c, sibling, 0).wait_recv()

    def edge_arrived(slot):
        each_side(lambda side: edge_pass(side, mine, slot, sibling, 0).wait_recv())

    each_side(lambda side: edge_copy(side, mine, 0).start())
    each_side(lambda side: edge_copy(side, 2, 2).start())
    pl.when(jnp.logical_not(is_d))(lambda: each_side(lambda side: edge_copy(side, slot_y, reach_y).start()))
    for c in range(CHUNKS):
        send_x(c).start()
        pl.when(jnp.logical_not(is_d))(lambda c=c: send_y(c).start())

    def prepare(t):
        row = lax.broadcasted_iota(jnp.int32, (planes, LANES), 0)
        lanes = lax.broadcasted_iota(jnp.int32, (planes, LANES), 1)
        col = lanes % NZ
        edge_z = jnp.logical_or(col == 0, col == NZ - 1)
        bottom = jnp.logical_and(t == 0, lanes < NZ)
        top = jnp.logical_and(t == tiles - 1, lanes >= NZ)
        first = jnp.logical_and(row == 0, jnp.logical_not(has[0]))
        last = jnp.logical_and(row == planes - 1, jnp.logical_not(has[1]))
        value = jnp.full((planes, LANES), outer + 6.0, jnp.float32)
        for walled in (edge_z, jnp.logical_or(bottom, top), first, last):
            value = value - jnp.where(walled, 1.0, 0.0)
        centre[t] = value

    loop(tiles, prepare)

    source_lane = lax.broadcasted_iota(jnp.int32, (2 * LANES, LANES), 0)
    target_lane = lax.broadcasted_iota(jnp.int32, (2 * LANES, LANES), 1)
    for which in range(3):
        for h in range(2):
            wanted = (target_lane // NZ) * LANES + h * NZ + target_lane % NZ + which
            hit = jnp.logical_and(source_lane == wanted, target_lane % NZ + which < NZ)
            c = (2 * which + h) * LANES
            moves[:, c:c + LANES] = jnp.where(hit, 1.0, 0.0).astype(jnp.bfloat16)

    def seam(value, keep_low):
        return jnp.where(low if keep_low else jnp.logical_not(low), pltpu.roll(value, NZ, 1), 0.0)

    per = half // CHUNKS

    def widen(slot, dst, c):
        pairs = range(c * per, (c + 1) * per)
        rows = [jnp.concatenate([slots[slot, o, part, :, k * LANES:(k + 1) * LANES] for part in range(2)], axis=1)
                for o in range(orbs) for k in pairs]
        rows += [halos[slot, side, g] for side in range(2) for g in range(c * per // GROUP, (c + 1) * per // GROUP)]
        moved = jnp.dot(jnp.concatenate(rows, axis=0), moves[...], preferred_element_type=jnp.float32)
        r = 0
        for o in range(orbs):
            for k in pairs:
                for n in range(6):
                    dst[o, n // 2, 2 * k + n % 2 + PAD, TOP:TOP + planes] = moved[r:r + planes, n * LANES:(n + 1) * LANES]
                r += planes
        for to in (TOP - WIDTH, TOP + planes):
            for k in pairs:
                for o in range(orbs):
                    for n in range(4):
                        dst[o, n // 2, 2 * k + n % 2 + PAD, to:to + WIDTH] = moved[r:r + WIDTH, n * LANES:(n + 1) * LANES]
                    r += WIDTH

    def pad_end(dst):
        for o in range(orbs):
            for which in range(2):
                for n in range(PAD):
                    dst[o, which, tiles + PAD + n] = seam(dst[o, which, PAD + n], True)

    def pad_start(dst):
        for o in range(orbs):
            for which in range(2):
                for n in range(PAD):
                    dst[o, which, n] = seam(dst[o, which, tiles + n], False)

    start = TOP - WIDTH
    ext = wide.shape[2]

    def gather(slot, src, fresh, first, count):
        if fresh:
            rows = edges[0, groups]
        else:
            rows = jnp.where(has[0], halos[slot, 0, groups].astype(jnp.float32), halos[slot, 1, groups].astype(jnp.float32))
        rows = -scale * rows[:orbs, :LANES].astype(jnp.float32)
        weights = [jnp.broadcast_to(rows[o:o + 1], (ext, LANES)) for o in range(orbs)]

        def body(t):
            at_t = t + PAD
            w = [weights[o] * src[o, 0, at_t, start:start + ext] for o in range(orbs)]
            for n, (which, dx, dy) in enumerate(WIDE):
                value = None if fresh else wide[n, at_t]
                for o in range(orbs):
                    term = w[o] * src[o, which, at_t + dy, start + dx:start + dx + ext]
                    value = term if value is None else value + term
                wide[n, at_t] = value
            w = [weights[o][:planes] * src[o, 0, at_t, TOP:TOP + planes] for o in range(orbs)]
            for n, (which, dy) in enumerate(FLAT):
                value = None if fresh else gram[n, at_t]
                for o in range(orbs):
                    term = w[o] * src[o, which, at_t + dy, TOP:TOP + planes]
                    value = term if value is None else value + term
                gram[n, at_t] = value
        loop(count, body, 2 if count % 2 == 0 else 1, first)

    def finish(t, i):
        at_t = t + PAD

        def orbital(which, dx=0, dy=0):
            return own[i, which, at_t + dy, TOP + dx:TOP + dx + planes]

        def flat(n, dy=0):
            return gram[n, at_t + dy]

        def deep(n, dx=0, dy=0):
            return wide[n, at_t + dy, WIDTH + dx:WIDTH + dx + planes]

        mid = orbital(0)
        near = orbital(0, 1) * deep(0) + orbital(0, -1) * deep(0, -1)
        near = near + (orbital(0, 0, 1) * flat(1) + orbital(0, 0, -1) * flat(1, -1))
        near = near + orbital(1) * flat(3)
        far = orbital(0, 2) * deep(1) + orbital(0, -2) * deep(1, -2)
        far = far + (orbital(0, 0, 2) * flat(2) + orbital(0, 0, -2) * flat(2, -2))
        far = far + orbital(2) * flat(4)
        diag = orbital(0, 1, 1) * deep(2) + orbital(0, -1, -1) * deep(2, -1, -1)
        diag = diag + (orbital(0, 1, -1) * deep(3) + orbital(0, -1, 1) * deep(3, -1, 1))
        diag = diag + (orbital(1, 1) * deep(4) + orbital(1, -1) * deep(5))
        diag = diag + (orbital(1, 0, 1) * flat(5) + orbital(1, 0, -1) * flat(6))
        back = orbital(0, -1) * deep(4, -1) + orbital(0, 1) * deep(5, 1)
        back = back + (orbital(0, 0, -1) * flat(5, -1) + orbital(0, 0, 1) * flat(6, 1))
        back = inner * (mid * flat(3)) + 2.0 * back
        rest[0, i, t] = centre[t] * (mid * flat(0)) + inner * near + (2.0 * diag + far)
        rest[1, i, t] = back
        rest[2, i, t] = mid * flat(4)

    def whole(slot, dst, fresh):
        for c in range(CHUNKS):
            widen(slot, dst, c)
        pad_start(dst)
        pad_end(dst)
        gather(slot, dst, fresh, 0, tiles)

    def edges_in(slot):
        edge_arrived(slot)

        @pl.when(slot == 2)
        def _():
            each_side(lambda side: edge_on(side).start())
            pl.when(is_b)(lambda: each_side(lambda side: edge_relay(side).start()))

    def chunk_in(slot, c):
        arrived(slot, c)

        @pl.when(slot == 2)
        def _():
            send_on(c).start()
            pl.when(is_b)(lambda: relay(c).start())

    edge_arrived(mine)
    whole(mine, own, True)

    def total(t, i):
        return rest[0, i, t] + pltpu.roll(rest[1, i, t], 1, 1) + pltpu.roll(rest[2, i, t], 2, 1)

    def pair_of(n):
        return lax.rem(n + PAD + half, half)

    def turn(n):
        k = pair_of(n)
        for i in range(orbs):
            for h in range(2):
                rest[0, i, 2 * k + h] = total(2 * k + h, i)

    def store(n):
        k = pair_of(n)
        for i in range(orbs):
            a, b = shuffle(rest[0, i, 2 * k], rest[0, i, 2 * k + 1])
            out_ref[i, :, lane_tile(k)] = a
            out_ref[i, :, lane_tile(k + half)] = b

    def apply(n):
        store(n - 2)
        turn(n - 1)
        k = pair_of(n)
        for h in range(2):
            for i in range(orbs):
                finish(2 * k + h, i)

    order = (by_kind(3, 1, 2, 1), by_kind(2, 2, 1, 2), by_kind(1, 3, 3, 3))

    def visit(n, c):
        slot = order[n]
        dst = vis.at[n % 2]
        if c == 0:
            edges_in(slot)
        chunk_in(slot, c)
        widen(slot, dst, c)
        if c == 0:
            pad_end(dst)
        first = 2 * per * c - PAD if c else 1
        final = c == CHUNKS - 1
        gather(slot, dst, False, first, (tiles if final else 2 * per * (c + 1) - PAD) - first)
        if final:
            pad_start(dst)
            gather(slot, dst, False, 0, 1)

    applied = 0
    for c in range(CHUNKS):
        visit(0, c)
    visit(1, 0)
    for c in range(CHUNKS):
        final = c == CHUNKS - 1
        if not final:
            visit(1, c + 1)
        visit(2, c)
        if final:
            for n, (which, dy) in enumerate(FLAT):
                if dy > 0:
                    for p in range(dy):
                        gram[n, PAD - 1 - p] = seam(gram[n, PAD + tiles - 1 - p], False)
                if dy < 0:
                    gram[n, PAD + tiles] = seam(gram[n, PAD], True)
            for n, (which, dx, dy) in enumerate(WIDE):
                if dy > 0:
                    wide[n, PAD - 1] = seam(wide[n, PAD + tiles - 1], False)
                if dy < 0:
                    wide[n, PAD + tiles] = seam(wide[n, PAD], True)
        done = half if final else max((2 * per * (c + 1) - PAD - 1) // 2 - PAD, 0)
        if done > applied:
            loop(done - applied, apply, 1, applied)
        applied = done
    store(half - 2)
    turn(half - 1)
    store(half - 1)

    each_side(lambda side: edge_copy(side, mine, 0).wait_send())
    each_side(lambda side: edge_copy(side, 2, 2).wait_send())
    each_side(lambda side: edge_on(side).wait_send())
    for c in range(CHUNKS):
        send_x(c).wait_send()
        send_on(c).wait_send()

    @pl.when(jnp.logical_not(is_d))
    def _():
        each_side(lambda side: edge_copy(side, slot_y, reach_y).wait_send())
        for c in range(CHUNKS):
            send_y(c).wait_send()

    @pl.when(is_b)
    def _():
        each_side(lambda side: edge_relay(side).wait_send())
        for c in range(CHUNKS):
            relay(c).wait_send()


def per_device(n_band, n_slab, orbitals, occupation):
    orbs, planes, cells = orbitals.shape
    tiles = cells // LANES
    ext = -(-(planes + 2 * WIDTH) // 8) * 8
    tall = planes + 2 * TOP + 8
    occ = occupation.reshape(1, orbs)
    f32, bf16 = jnp.float32, jnp.bfloat16
    rows, groups = GROUP * orbs * WIDTH, tiles // (2 * GROUP)
    padded = tiles + 2 * PAD + 1
    return pl.pallas_call(
        functools.partial(kernel, n_band, n_slab),
        out_shape=pltpu.VMEM(orbitals.shape, f32),
        in_specs=[pl.BlockSpec(memory_space=pl.ANY)] * 2,
        out_specs=pl.BlockSpec(memory_space=pltpu.VMEM),
        scratch_shapes=[
            pltpu.VMEM((SENDS, orbs, 2, planes, cells // 2), bf16),
            pltpu.VMEM((2, groups + 1, rows, 2 * LANES), bf16),
            pltpu.VMEM((SENDS, 2, groups + 1, rows, 2 * LANES), bf16),
            pltpu.VMEM((orbs, 3, padded, tall, LANES), f32),
            pltpu.VMEM((2, orbs, 3, padded, tall, LANES), f32),
            pltpu.VMEM((len(FLAT), padded, planes, LANES), f32),
            pltpu.VMEM((len(WIDE), padded, ext, LANES), f32),
            pltpu.VMEM((tiles, planes, LANES), f32),
            pltpu.VMEM((2 * LANES, 6 * LANES), bf16),
            pltpu.VMEM((3, orbs, tiles, planes, LANES), f32),
            pltpu.VMEM(occ.shape, bf16),
            pltpu.SemaphoreType.DMA((3,)),
            pltpu.SemaphoreType.DMA((SENDS, CHUNKS)),
            pltpu.SemaphoreType.DMA((SENDS, CHUNKS)),
            pltpu.SemaphoreType.DMA((SENDS + 2, 2)),
            pltpu.SemaphoreType.DMA((SENDS, 2)),
        ],
        compiler_params=pltpu.CompilerParams(collective_id=0, has_side_effects=True),
        name="exchange",
    )(orbitals, occ)


def solution(mesh):
    in_specs = (P("band", "slab", None), P("band"))
    out_specs = P("band", "slab", None)
    return jax.shard_map(
        functools.partial(per_device, mesh.shape["band"], mesh.shape["slab"]),
        mesh=mesh, in_specs=in_specs, out_specs=out_specs, check_vma=False,
    )
```

```python
import functools
import math

import jax
import jax.numpy as jnp
from jax import lax
from jax.experimental import pallas as pl
from jax.experimental.pallas import tpu as pltpu
from jax.sharding import PartitionSpec as P

NZ = 64
STEPS = 3
LANES = 128
WIDTH = 2
PAD = 2
GROUP = 4
CUTS = (0, 4, 8, 12, 16)
CHUNKS = len(CUTS) - 1
SENDS = STEPS + 1
TOP = 8
FLAT = ((0, 0), (0, 1), (0, 2), (1, 0), (2, 0), (1, 1), (1, -1))
WIDE = ((0, 1, 0), (0, 2, 0), (0, 1, 1), (0, 1, -1), (1, 1, 0), (1, -1, 0))
MESH = pl.DeviceIdType.MESH


screening = 0.5
ratio_mid = (12.0 + 2.0 * screening) / 12.0
root_term = math.sqrt(ratio_mid * ratio_mid - 1.0)
decay_ratio = ratio_mid - root_term
coeff_zero = 1.0 / (6.0 * root_term)
coeff_one = -2.0 * decay_ratio * coeff_zero
coeff_two = 2.0 * decay_ratio * decay_ratio * coeff_zero

scale = coeff_two / 18.0
inner = -coeff_one / 6.0 / scale
outer = (coeff_zero - coeff_two) / scale


def loop(count, body, unroll=1, start=0):
    lax.fori_loop(start, start + count, lambda i, c: (body(i), c)[1], 0, unroll=unroll)


def lane_tile(t):
    return pl.ds(pl.multiple_of(t * LANES, LANES), LANES)


def kernel(n_band, n_slab, orb_ref, occ_ref, out_ref, slots, edges, halos, own, vis, gram, wide, centre,
           moves, rest, occ, factors, load_sem, send_sem, recv_sem, edge_send, edge_recv):
    orbs, planes, cells = orb_ref.shape
    tiles = cells // LANES
    half = tiles // 2
    groups = half // GROUP
    mine = 0
    bounds = [half * n // CUTS[-1] for n in CUTS]
    band, slab = lax.axis_index("band"), lax.axis_index("slab")
    kind = lax.rem(band, 4)
    is_b, is_d = kind == 1, kind == 3

    def by_kind(a, b, c, d):
        return jnp.where(kind == 0, a, jnp.where(kind == 1, b, jnp.where(kind == 2, c, d)))

    def at(by, side=0):
        return {"band": lax.rem(band + by + n_band, n_band), "slab": slab + side}

    sibling = at(by_kind(1, -1, 1, -1))
    has = (slab > 0, slab < n_slab - 1)
    step_of = (-1, 1)
    reach_y, slot_y = by_kind(1, 3, 1, 1), by_kind(1, 3, 1, 1)
    slot_pass = by_kind(3, 1, 3, 1)

    loads = [pltpu.make_async_copy(orb_ref.at[:, :, part * half * LANES:(part + 1) * half * LANES],
                                   slots.at[mine, :, part], load_sem.at[part]) for part in range(2)]
    loads.append(pltpu.make_async_copy(occ_ref, occ, load_sem.at[2]))
    for load in loads:
        load.start()

    barrier = pltpu.get_barrier_semaphore()
    sides = has[0].astype(jnp.int32) + has[1].astype(jnp.int32)
    straight = {0: (1, -2, -3), 1: (-1, -2), 2: (-2, 1, -1), 3: (-1, -2)}
    slanted = {0: (-2, -3), 1: (-1, -2), 2: (-2,), 3: (-1, -2)}

    def greet(by, side=0):
        pl.semaphore_signal(barrier, inc=1, device_id=at(by, side), device_id_type=MESH)

    for which in range(4):
        @pl.when(kind == which)
        def _(which=which):
            for by in sorted(straight[which]):
                greet(by)
            for side in range(2):
                @pl.when(has[side])
                def _(side=side):
                    for by in sorted(slanted[which]) + [0]:
                        greet(by, step_of[side])

    lane = lax.broadcasted_iota(jnp.int32, (1, LANES), 1)
    low = lane < NZ
    column = lane % NZ

    def shuffle(a, b):
        turned = pltpu.roll(jnp.where(low, b, a), NZ, 1)
        return jnp.where(low, a, turned), jnp.where(low, turned, b)

    for load in loads:
        load.wait()
    pl.semaphore_wait(barrier, by_kind(2, 4, 2, 2) + sides * by_kind(3, 3, 3, 2))

    def edge_copy(side, slot, by):
        return pltpu.make_async_remote_copy(
            src_ref=edges.at[side], dst_ref=halos.at[slot, 1 - side],
            send_sem=edge_send.at[slot, side], recv_sem=edge_recv.at[slot, 1 - side],
            device_id=at(by, step_of[side]), device_id_type=MESH)

    def edge_pass(side, src, slot, device, sem):
        return pltpu.make_async_remote_copy(
            src_ref=halos.at[src, side], dst_ref=halos.at[slot, side],
            send_sem=edge_send.at[sem, side], recv_sem=edge_recv.at[slot, side],
            device_id=device, device_id_type=MESH)

    def piece(ref, slot, c):
        return ref.at[slot, :, :, :, bounds[c] * LANES:bounds[c + 1] * LANES]

    def block_copy(src, slot, c, device, sem):
        return pltpu.make_async_remote_copy(
            src_ref=piece(slots, src, c), dst_ref=piece(slots, slot, c), send_sem=send_sem.at[sem, c],
            recv_sem=recv_sem.at[slot, c], device_id=device, device_id_type=MESH)

    def each_side(action):
        for side in range(2):
            pl.when(has[side])(functools.partial(action, side))

    def send_x(c):
        return block_copy(mine, 2, c, at(2), 0)

    def send_y(c):
        return block_copy(mine, slot_y, c, at(reach_y), 1)

    def send_on(c):
        return block_copy(2, slot_pass, c, sibling, 2)

    def relay(c):
        return block_copy(2, 3, c, at(1), 3)

    def edge_on(side):
        return edge_pass(side, 2, slot_pass, sibling, SENDS)

    def edge_relay(side):
        return edge_pass(side, 2, 3, at(1), SENDS + 1)

    def arrived(slot, c):
        block_copy(mine, slot, c, sibling, 0).wait_recv()

    def edge_arrived(slot):
        each_side(lambda side: edge_pass(side, mine, slot, sibling, 0).wait_recv())

    send_x(0).start()
    for side in range(2):
        rows = [jnp.broadcast_to(occ[:, o:o + 1].astype(jnp.float32), (1, 2 * LANES)) for o in range(orbs)]
        rows.append(jnp.zeros((edges.shape[2] - orbs, 2 * LANES), jnp.float32))
        edges[side, groups] = jnp.concatenate(rows, axis=0).astype(jnp.bfloat16)

    def cut(g):
        parts = ([], [])
        for n in range(GROUP):
            for o in range(orbs):
                pair = [slots[mine, o, part, :, lane_tile(GROUP * g + n)].astype(jnp.float32) for part in range(2)]
                for side in range(2):
                    at_plane = 0 if side == 0 else planes - WIDTH
                    parts[side].append(jnp.concatenate([p[at_plane:at_plane + WIDTH] for p in pair], axis=1))
        for side in range(2):
            edges[side, g] = jnp.concatenate(parts[side], axis=0).astype(jnp.bfloat16)

    loop(groups, cut)

    for side in range(2):
        @pl.when(jnp.logical_not(has[side]))
        def _(side=side):
            halos[:, side] = jnp.zeros(halos.shape[:1] + halos.shape[2:], jnp.bfloat16)

    each_side(lambda side: edge_copy(side, mine, 0).start())
    each_side(lambda side: edge_copy(side, 2, 2).start())
    pl.when(jnp.logical_not(is_d))(lambda: each_side(lambda side: edge_copy(side, slot_y, reach_y).start()))
    for c in range(CHUNKS):
        if c > 0:
            send_x(c).start()
        pl.when(jnp.logical_not(is_d))(lambda c=c: send_y(c).start())

    def prepare(t):
        row = lax.broadcasted_iota(jnp.int32, (planes, LANES), 0)
        lanes = lax.broadcasted_iota(jnp.int32, (planes, LANES), 1)
        col = lanes % NZ
        edge_z = jnp.logical_or(col == 0, col == NZ - 1)
        bottom = jnp.logical_and(t == 0, lanes < NZ)
        top = jnp.logical_and(t == tiles - 1, lanes >= NZ)
        first = jnp.logical_and(row == 0, jnp.logical_not(has[0]))
        last = jnp.logical_and(row == planes - 1, jnp.logical_not(has[1]))
        value = jnp.full((planes, LANES), outer + 6.0, jnp.float32)
        for walled in (edge_z, jnp.logical_or(bottom, top), first, last):
            value = value - jnp.where(walled, 1.0, 0.0)
        centre[t] = value

    loop(tiles, prepare)

    source_lane = lax.broadcasted_iota(jnp.int32, (2 * LANES, LANES), 0)
    target_lane = lax.broadcasted_iota(jnp.int32, (2 * LANES, LANES), 1)
    for which in range(3):
        for h in range(2):
            wanted = (target_lane // NZ) * LANES + h * NZ + target_lane % NZ + which
            hit = jnp.logical_and(source_lane == wanted, target_lane % NZ + which < NZ)
            c = (2 * which + h) * LANES
            moves[:, c:c + LANES] = jnp.where(hit, 1.0, 0.0).astype(jnp.bfloat16)

    def seam(value, keep_low):
        return jnp.where(low if keep_low else jnp.logical_not(low), pltpu.roll(value, NZ, 1), 0.0)

    def widen(slot, dst, c):
        pairs = range(bounds[c], bounds[c + 1])
        near = range(bounds[c] // GROUP, -(-bounds[c + 1] // GROUP))
        rows = [jnp.concatenate([slots[slot, o, part, :, k * LANES:(k + 1) * LANES] for part in range(2)], axis=1)
                for o in range(orbs) for k in pairs]
        rows += [halos[slot, side, g] for side in range(2) for g in near]
        moved = jnp.dot(jnp.concatenate(rows, axis=0), moves[...], preferred_element_type=jnp.float32)
        r = 0
        for o in range(orbs):
            for k in pairs:
                for n in range(6):
                    dst[o, n // 2, 2 * k + n % 2 + PAD, TOP:TOP + planes] = moved[r:r + planes, n * LANES:(n + 1) * LANES]
                r += planes
        for to in (TOP - WIDTH, TOP + planes):
            for k in range(near[0] * GROUP, (near[-1] + 1) * GROUP):
                for o in range(orbs):
                    for n in range(4 if k in pairs else 0):
                        dst[o, n // 2, 2 * k + n % 2 + PAD, to:to + WIDTH] = moved[r:r + WIDTH, n * LANES:(n + 1) * LANES]
                    r += WIDTH

    def pad_end(dst):
        for o in range(orbs):
            for which in range(2):
                for n in range(PAD):
                    dst[o, which, tiles + PAD + n] = seam(dst[o, which, PAD + n], True)

    def pad_start(dst):
        for o in range(orbs):
            for which in range(2):
                for n in range(PAD):
                    dst[o, which, n] = seam(dst[o, which, tiles + n], False)

    start = TOP - WIDTH
    ext = wide.shape[2]

    def weigh(slot, fresh):
        if fresh:
            rows = edges[0, groups]
        else:
            rows = jnp.where(has[0], halos[slot, 0, groups].astype(jnp.float32), halos[slot, 1, groups].astype(jnp.float32))
        rows = -scale * rows[:orbs, :LANES].astype(jnp.float32)
        for o in range(orbs):
            factors[slot, o] = jnp.broadcast_to(rows[o:o + 1], (8, LANES))

    def gather(slot, src, fresh, first, count):
        weights = [jnp.concatenate([factors[slot, o]] * (ext // 8), axis=0) for o in range(orbs)]

        def body(t):
            at_t = t + PAD
            w = [weights[o] * src[o, 0, at_t, start:start + ext] for o in range(orbs)]
            for n, (which, dx, dy) in enumerate(WIDE):
                value = None if fresh else wide[n, at_t]
                for o in range(orbs):
                    term = w[o] * src[o, which, at_t + dy, start + dx:start + dx + ext]
                    value = term if value is None else value + term
                wide[n, at_t] = value
            w = [weights[o][:planes] * src[o, 0, at_t, TOP:TOP + planes] for o in range(orbs)]
            for n, (which, dy) in enumerate(FLAT):
                value = None if fresh else gram[n, at_t]
                for o in range(orbs):
                    term = w[o] * src[o, which, at_t + dy, TOP:TOP + planes]
                    value = term if value is None else value + term
                gram[n, at_t] = value
        loop(count, body, count if count < tiles else 4, first)

    def finish(t, i):
        at_t = t + PAD

        def orbital(which, dx=0, dy=0):
            return own[i, which, at_t + dy, TOP + dx:TOP + dx + planes]

        def flat(n, dy=0):
            return gram[n, at_t + dy]

        def deep(n, dx=0, dy=0):
            return wide[n, at_t + dy, WIDTH + dx:WIDTH + dx + planes]

        mid = orbital(0)
        near = orbital(0, 1) * deep(0) + orbital(0, -1) * deep(0, -1)
        near = near + (orbital(0, 0, 1) * flat(1) + orbital(0, 0, -1) * flat(1, -1))
        near = near + orbital(1) * flat(3)
        far = orbital(0, 2) * deep(1) + orbital(0, -2) * deep(1, -2)
        far = far + (orbital(0, 0, 2) * flat(2) + orbital(0, 0, -2) * flat(2, -2))
        far = far + orbital(2) * flat(4)
        diag = orbital(0, 1, 1) * deep(2) + orbital(0, -1, -1) * deep(2, -1, -1)
        diag = diag + (orbital(0, 1, -1) * deep(3) + orbital(0, -1, 1) * deep(3, -1, 1))
        diag = diag + (orbital(1, 1) * deep(4) + orbital(1, -1) * deep(5))
        diag = diag + (orbital(1, 0, 1) * flat(5) + orbital(1, 0, -1) * flat(6))
        back = orbital(0, -1) * deep(4, -1) + orbital(0, 1) * deep(5, 1)
        back = back + (orbital(0, 0, -1) * flat(5, -1) + orbital(0, 0, 1) * flat(6, 1))
        back = inner * (mid * flat(3)) + 2.0 * back
        rest[0, i, t] = centre[t] * (mid * flat(0)) + inner * near + (2.0 * diag + far)
        rest[1, i, t] = back
        rest[2, i, t] = mid * flat(4)

    def whole(slot, dst, fresh):
        for c in range(CHUNKS):
            widen(slot, dst, c)
        pad_start(dst)
        pad_end(dst)
        gather(slot, dst, fresh, 0, tiles)

    def edges_in(slot):
        edge_arrived(slot)

        @pl.when(slot == 2)
        def _():
            each_side(lambda side: edge_on(side).start())
            pl.when(is_b)(lambda: each_side(lambda side: edge_relay(side).start()))

    def chunk_in(slot, c):
        arrived(slot, c)

        @pl.when(slot == 2)
        def _():
            send_on(c).start()
            pl.when(is_b)(lambda: relay(c).start())

    edge_arrived(mine)
    weigh(mine, True)
    whole(mine, own, True)

    def total(t, i):
        return rest[0, i, t] + pltpu.roll(rest[1, i, t], 1, 1) + pltpu.roll(rest[2, i, t], 2, 1)

    def pair_of(n):
        return lax.rem(n + PAD + half, half)

    def turn(n):
        k = pair_of(n)
        for i in range(orbs):
            for h in range(2):
                rest[0, i, 2 * k + h] = total(2 * k + h, i)

    def store(n):
        k = pair_of(n)
        for i in range(orbs):
            a, b = shuffle(rest[0, i, 2 * k], rest[0, i, 2 * k + 1])
            out_ref[i, :, lane_tile(k)] = a
            out_ref[i, :, lane_tile(k + half)] = b

    def apply(n):
        store(n - 2)
        turn(n - 1)
        k = pair_of(n)
        for h in range(2):
            for i in range(orbs):
                finish(2 * k + h, i)

    order = (by_kind(3, 1, 2, 1), by_kind(2, 2, 1, 2), by_kind(1, 3, 3, 3))

    def visit(n, c):
        slot = order[n]
        dst = vis.at[n % 2]
        if c == 0:
            edges_in(slot)
            weigh(slot, False)
        chunk_in(slot, c)
        widen(slot, dst, c)
        if c == 0:
            pad_end(dst)
        first = 2 * bounds[c] - PAD if c else 1
        final = c == CHUNKS - 1
        gather(slot, dst, False, first, (tiles if final else 2 * bounds[c + 1] - PAD) - first)
        if final:
            pad_start(dst)
            gather(slot, dst, False, 0, 1)

    def direct_sent():
        each_side(lambda side: edge_copy(side, mine, 0).wait_send())
        each_side(lambda side: edge_copy(side, 2, 2).wait_send())
        each_side(lambda side: edge_on(side).wait_send())
        pl.when(is_b)(lambda: each_side(lambda side: edge_relay(side).wait_send()))
        for c in range(CHUNKS):
            send_x(c).wait_send()

        @pl.when(jnp.logical_not(is_d))
        def _():
            each_side(lambda side: edge_copy(side, slot_y, reach_y).wait_send())
            for c in range(CHUNKS):
                send_y(c).wait_send()

    applied = 0
    for c in range(CHUNKS):
        visit(0, c)
    visit(1, 0)
    for c in range(CHUNKS):
        final = c == CHUNKS - 1
        if not final:
            visit(1, c + 1)
        else:
            direct_sent()
        visit(2, c)
        if final:
            for n, (which, dy) in enumerate(FLAT):
                if dy > 0:
                    for p in range(dy):
                        gram[n, PAD - 1 - p] = seam(gram[n, PAD + tiles - 1 - p], False)
                if dy < 0:
                    gram[n, PAD + tiles] = seam(gram[n, PAD], True)
            for n, (which, dx, dy) in enumerate(WIDE):
                if dy > 0:
                    wide[n, PAD - 1] = seam(wide[n, PAD + tiles - 1], False)
                if dy < 0:
                    wide[n, PAD + tiles] = seam(wide[n, PAD], True)
        done = half if final else max((2 * bounds[c + 1] - PAD - 1) // 2 - PAD, 0)
        if done > applied:
            loop(done - applied, apply, 1, applied)
        applied = done
    store(half - 2)
    turn(half - 1)
    store(half - 1)

    for c in range(CHUNKS):
        send_on(c).wait_send()

        pl.when(is_b)(lambda c=c: relay(c).wait_send())


def per_device(n_band, n_slab, orbitals, occupation):
    orbs, planes, cells = orbitals.shape
    tiles = cells // LANES
    ext = -(-(planes + 2 * WIDTH) // 8) * 8
    tall = planes + 2 * TOP + 8
    occ = occupation.reshape(1, orbs)
    f32, bf16 = jnp.float32, jnp.bfloat16
    rows, groups = GROUP * orbs * WIDTH, tiles // (2 * GROUP)
    padded = tiles + 2 * PAD
    return pl.pallas_call(
        functools.partial(kernel, n_band, n_slab),
        out_shape=pltpu.VMEM(orbitals.shape, f32),
        in_specs=[pl.BlockSpec(memory_space=pl.ANY)] * 2,
        out_specs=pl.BlockSpec(memory_space=pltpu.VMEM),
        scratch_shapes=[
            pltpu.VMEM((SENDS, orbs, 2, planes, cells // 2), bf16),
            pltpu.VMEM((2, groups + 1, rows, 2 * LANES), bf16),
            pltpu.VMEM((SENDS, 2, groups + 1, rows, 2 * LANES), bf16),
            pltpu.VMEM((orbs, 3, padded, tall, LANES), f32),
            pltpu.VMEM((2, orbs, 3, padded, tall, LANES), f32),
            pltpu.VMEM((len(FLAT), padded, planes, LANES), f32),
            pltpu.VMEM((len(WIDE), padded, ext, LANES), f32),
            pltpu.VMEM((tiles, planes, LANES), f32),
            pltpu.VMEM((2 * LANES, 6 * LANES), bf16),
            pltpu.VMEM((3, orbs, tiles, planes, LANES), f32),
            pltpu.VMEM(occ.shape, bf16),
            pltpu.VMEM((SENDS, orbs, 8, LANES), f32),
            pltpu.SemaphoreType.DMA((3,)),
            pltpu.SemaphoreType.DMA((SENDS, CHUNKS)),
            pltpu.SemaphoreType.DMA((SENDS, CHUNKS)),
            pltpu.SemaphoreType.DMA((SENDS + 2, 2)),
            pltpu.SemaphoreType.DMA((SENDS, 2)),
        ],
        compiler_params=pltpu.CompilerParams(collective_id=0, has_side_effects=True),
        name="exchange",
    )(orbitals, occ)


def solution(mesh):
    in_specs = (P("band", "slab", None), P("band"))
    out_specs = P("band", "slab", None)
    return jax.shard_map(
        functools.partial(per_device, mesh.shape["band"], mesh.shape["slab"]),
        mesh=mesh, in_specs=in_specs, out_specs=out_specs, check_vma=False,
    )
```

```python
import functools
import math

import jax
import jax.numpy as jnp
from jax import lax
from jax.experimental import pallas as pl
from jax.experimental.pallas import tpu as pltpu
from jax.sharding import PartitionSpec as P

NZ = 64
STEPS = 3
LANES = 128
WIDTH = 2
PAD = 2
GROUP = 4
CUTS = (0, 4, 8, 12, 16)
CHUNKS = len(CUTS) - 1
SENDS = STEPS + 1
TOP = 8
FLAT = ((0, 0), (0, 1), (0, 2), (1, 0), (2, 0), (1, 1), (1, -1))
WIDE = ((0, 1, 0), (0, 2, 0), (0, 1, 1), (0, 1, -1), (1, 1, 0), (1, -1, 0))
MESH = pl.DeviceIdType.MESH


screening = 0.5
ratio_mid = (12.0 + 2.0 * screening) / 12.0
root_term = math.sqrt(ratio_mid * ratio_mid - 1.0)
decay_ratio = ratio_mid - root_term
coeff_zero = 1.0 / (6.0 * root_term)
coeff_one = -2.0 * decay_ratio * coeff_zero
coeff_two = 2.0 * decay_ratio * decay_ratio * coeff_zero

scale = coeff_two / 18.0
inner = -coeff_one / 6.0 / scale
outer = (coeff_zero - coeff_two) / scale


def loop(count, body, unroll=1, start=0):
    lax.fori_loop(start, start + count, lambda i, c: (body(i), c)[1], 0, unroll=unroll)


def lane_tile(t):
    return pl.ds(pl.multiple_of(t * LANES, LANES), LANES)


def kernel(n_band, n_slab, orb_ref, occ_ref, out_ref, slots, edges, halos, own, vis, gram, wide, centre,
           moves, rest, occ, factors, load_sem, send_sem, recv_sem, edge_send, edge_recv):
    orbs, planes, cells = orb_ref.shape
    tiles = cells // LANES
    half = tiles // 2
    groups = half // GROUP
    mine = 0
    bounds = [half * n // CUTS[-1] for n in CUTS]
    band, slab = lax.axis_index("band"), lax.axis_index("slab")
    kind = lax.rem(band, 4)
    is_b, is_d = kind == 1, kind == 3

    def by_kind(a, b, c, d):
        return jnp.where(kind == 0, a, jnp.where(kind == 1, b, jnp.where(kind == 2, c, d)))

    def at(by, side=0):
        return {"band": lax.rem(band + by + n_band, n_band), "slab": slab + side}

    sibling = at(by_kind(1, -1, 1, -1))
    has = (slab > 0, slab < n_slab - 1)
    step_of = (-1, 1)
    reach_y, slot_y = by_kind(1, 3, 1, 1), by_kind(1, 3, 1, 1)
    slot_pass = by_kind(3, 1, 3, 1)

    loads = [pltpu.make_async_copy(orb_ref.at[:, :, part * half * LANES:(part + 1) * half * LANES],
                                   slots.at[mine, :, part], load_sem.at[part]) for part in range(2)]
    loads.append(pltpu.make_async_copy(occ_ref, occ, load_sem.at[2]))
    for load in loads:
        load.start()

    barrier = pltpu.get_barrier_semaphore()
    sides = has[0].astype(jnp.int32) + has[1].astype(jnp.int32)
    straight = {0: (1, -2, -3), 1: (-1, -2), 2: (-2, 1, -1), 3: (-1, -2)}
    slanted = {0: (-2, -3), 1: (-1, -2), 2: (-2,), 3: (-1, -2)}

    def greet(by, side=0):
        pl.semaphore_signal(barrier, inc=1, device_id=at(by, side), device_id_type=MESH)

    for which in range(4):
        @pl.when(kind == which)
        def _(which=which):
            for by in sorted(straight[which]):
                greet(by)
            for side in range(2):
                @pl.when(has[side])
                def _(side=side):
                    for by in sorted(slanted[which]) + [0]:
                        greet(by, step_of[side])

    lane = lax.broadcasted_iota(jnp.int32, (1, LANES), 1)
    low = lane < NZ
    column = lane % NZ

    def shuffle(a, b):
        turned = pltpu.roll(jnp.where(low, b, a), NZ, 1)
        return jnp.where(low, a, turned), jnp.where(low, turned, b)

    for load in loads:
        load.wait()
    pl.semaphore_wait(barrier, by_kind(2, 4, 2, 2) + sides * by_kind(3, 3, 3, 2))

    def edge_copy(side, slot, by):
        return pltpu.make_async_remote_copy(
            src_ref=edges.at[side], dst_ref=halos.at[slot, 1 - side],
            send_sem=edge_send.at[slot, side], recv_sem=edge_recv.at[slot, 1 - side],
            device_id=at(by, step_of[side]), device_id_type=MESH)

    def edge_pass(side, src, slot, device, sem):
        return pltpu.make_async_remote_copy(
            src_ref=halos.at[src, side], dst_ref=halos.at[slot, side],
            send_sem=edge_send.at[sem, side], recv_sem=edge_recv.at[slot, side],
            device_id=device, device_id_type=MESH)

    def piece(ref, slot, c):
        return ref.at[slot, :, :, :, bounds[c] * LANES:bounds[c + 1] * LANES]

    def block_copy(src, slot, c, device, sem):
        return pltpu.make_async_remote_copy(
            src_ref=piece(slots, src, c), dst_ref=piece(slots, slot, c), send_sem=send_sem.at[sem, c],
            recv_sem=recv_sem.at[slot, c], device_id=device, device_id_type=MESH)

    def each_side(action):
        for side in range(2):
            pl.when(has[side])(functools.partial(action, side))

    def send_x(c):
        return block_copy(mine, 2, c, at(2), 0)

    def send_y(c):
        return block_copy(mine, slot_y, c, at(reach_y), 1)

    def send_on(c):
        return block_copy(2, slot_pass, c, sibling, 2)

    def relay(c):
        return block_copy(2, 3, c, at(1), 3)

    def edge_on(side):
        return edge_pass(side, 2, slot_pass, sibling, SENDS)

    def edge_relay(side):
        return edge_pass(side, 2, 3, at(1), SENDS + 1)

    def arrived(slot, c):
        block_copy(mine, slot, c, sibling, 0).wait_recv()

    def edge_arrived(slot):
        each_side(lambda side: edge_pass(side, mine, slot, sibling, 0).wait_recv())

    send_x(0).start()
    for side in range(2):
        rows = [jnp.broadcast_to(occ[:, o:o + 1].astype(jnp.float32), (1, 2 * LANES)) for o in range(orbs)]
        rows.append(jnp.zeros((edges.shape[2] - orbs, 2 * LANES), jnp.float32))
        edges[side, groups] = jnp.concatenate(rows, axis=0).astype(jnp.bfloat16)

    def cut(g):
        parts = ([], [])
        for n in range(GROUP):
            for o in range(orbs):
                pair = [slots[mine, o, part, :, lane_tile(GROUP * g + n)].astype(jnp.float32) for part in range(2)]
                for side in range(2):
                    at_plane = 0 if side == 0 else planes - WIDTH
                    parts[side].append(jnp.concatenate([p[at_plane:at_plane + WIDTH] for p in pair], axis=1))
        for side in range(2):
            edges[side, g] = jnp.concatenate(parts[side], axis=0).astype(jnp.bfloat16)

    loop(groups, cut)

    for side in range(2):
        @pl.when(jnp.logical_not(has[side]))
        def _(side=side):
            halos[:, side] = jnp.zeros(halos.shape[:1] + halos.shape[2:], jnp.bfloat16)

    each_side(lambda side: edge_copy(side, mine, 0).start())
    each_side(lambda side: edge_copy(side, 2, 2).start())
    pl.when(jnp.logical_not(is_d))(lambda: each_side(lambda side: edge_copy(side, slot_y, reach_y).start()))
    for c in range(CHUNKS):
        if c > 0:
            send_x(c).start()
        pl.when(jnp.logical_not(is_d))(lambda c=c: send_y(c).start())

    def prepare(t):
        row = lax.broadcasted_iota(jnp.int32, (planes, LANES), 0)
        lanes = lax.broadcasted_iota(jnp.int32, (planes, LANES), 1)
        col = lanes % NZ
        edge_z = jnp.logical_or(col == 0, col == NZ - 1)
        bottom = jnp.logical_and(t == 0, lanes < NZ)
        top = jnp.logical_and(t == tiles - 1, lanes >= NZ)
        first = jnp.logical_and(row == 0, jnp.logical_not(has[0]))
        last = jnp.logical_and(row == planes - 1, jnp.logical_not(has[1]))
        value = jnp.full((planes, LANES), outer + 6.0, jnp.float32)
        for walled in (edge_z, jnp.logical_or(bottom, top), first, last):
            value = value - jnp.where(walled, 1.0, 0.0)
        centre[t] = value

    loop(tiles, prepare)

    source_lane = lax.broadcasted_iota(jnp.int32, (2 * LANES, LANES), 0)
    target_lane = lax.broadcasted_iota(jnp.int32, (2 * LANES, LANES), 1)
    for which in range(3):
        for h in range(2):
            wanted = (target_lane // NZ) * LANES + h * NZ + target_lane % NZ + which
            hit = jnp.logical_and(source_lane == wanted, target_lane % NZ + which < NZ)
            c = (2 * which + h) * LANES
            moves[:, c:c + LANES] = jnp.where(hit, 1.0, 0.0).astype(jnp.bfloat16)

    def seam(value, keep_low):
        return jnp.where(low if keep_low else jnp.logical_not(low), pltpu.roll(value, NZ, 1), 0.0)

    def widen(slot, dst, c):
        pairs = range(bounds[c], bounds[c + 1])
        near = range(bounds[c] // GROUP, -(-bounds[c + 1] // GROUP))
        rows = [jnp.concatenate([slots[slot, o, part, :, k * LANES:(k + 1) * LANES] for part in range(2)], axis=1)
                for o in range(orbs) for k in pairs]
        rows += [halos[slot, side, g] for side in range(2) for g in near]
        moved = jnp.dot(jnp.concatenate(rows, axis=0), moves[...], preferred_element_type=jnp.float32)
        r = 0
        for o in range(orbs):
            for k in pairs:
                for n in range(6):
                    dst[o, n // 2, 2 * k + n % 2 + PAD, TOP:TOP + planes] = moved[r:r + planes, n * LANES:(n + 1) * LANES]
                r += planes
        for to in (TOP - WIDTH, TOP + planes):
            for k in range(near[0] * GROUP, (near[-1] + 1) * GROUP):
                for o in range(orbs):
                    for n in range(4 if k in pairs else 0):
                        dst[o, n // 2, 2 * k + n % 2 + PAD, to:to + WIDTH] = moved[r:r + WIDTH, n * LANES:(n + 1) * LANES]
                    r += WIDTH

    def pad_end(dst):
        for o in range(orbs):
            for which in range(2):
                for n in range(PAD):
                    dst[o, which, tiles + PAD + n] = seam(dst[o, which, PAD + n], True)

    def pad_start(dst):
        for o in range(orbs):
            for which in range(2):
                for n in range(PAD):
                    dst[o, which, n] = seam(dst[o, which, tiles + n], False)

    start = TOP - WIDTH
    ext = wide.shape[2]

    def weigh(slot, fresh):
        if fresh:
            rows = edges[0, groups]
        else:
            rows = jnp.where(has[0], halos[slot, 0, groups].astype(jnp.float32), halos[slot, 1, groups].astype(jnp.float32))
        rows = -scale * rows[:orbs, :LANES].astype(jnp.float32)
        for o in range(orbs):
            factors[slot, o] = jnp.broadcast_to(rows[o:o + 1], (8, LANES))

    def gather(slot, src, fresh, first, count):
        weights = [jnp.concatenate([factors[slot, o]] * (ext // 8), axis=0) for o in range(orbs)]

        def body(t):
            at_t = t + PAD
            w = [weights[o] * src[o, 0, at_t, start:start + ext] for o in range(orbs)]
            for n, (which, dx, dy) in enumerate(WIDE):
                value = None if fresh else wide[n, at_t]
                for o in range(orbs):
                    term = w[o] * src[o, which, at_t + dy, start + dx:start + dx + ext]
                    value = term if value is None else value + term
                wide[n, at_t] = value
            w = [weights[o][:planes] * src[o, 0, at_t, TOP:TOP + planes] for o in range(orbs)]
            for n, (which, dy) in enumerate(FLAT):
                value = None if fresh else gram[n, at_t]
                for o in range(orbs):
                    term = w[o] * src[o, which, at_t + dy, TOP:TOP + planes]
                    value = term if value is None else value + term
                gram[n, at_t] = value
        loop(count, body, count if count < tiles else 4, first)

    def finish(t, i):
        at_t = t + PAD

        def orbital(which, dx=0, dy=0):
            return own[i, which, at_t + dy, TOP + dx:TOP + dx + planes]

        def flat(n, dy=0):
            return gram[n, at_t + dy]

        def deep(n, dx=0, dy=0):
            return wide[n, at_t + dy, WIDTH + dx:WIDTH + dx + planes]

        mid = orbital(0)
        near = orbital(0, 1) * deep(0) + orbital(0, -1) * deep(0, -1)
        near = near + (orbital(0, 0, 1) * flat(1) + orbital(0, 0, -1) * flat(1, -1))
        near = near + orbital(1) * flat(3)
        far = orbital(0, 2) * deep(1) + orbital(0, -2) * deep(1, -2)
        far = far + (orbital(0, 0, 2) * flat(2) + orbital(0, 0, -2) * flat(2, -2))
        far = far + orbital(2) * flat(4)
        diag = orbital(0, 1, 1) * deep(2) + orbital(0, -1, -1) * deep(2, -1, -1)
        diag = diag + (orbital(0, 1, -1) * deep(3) + orbital(0, -1, 1) * deep(3, -1, 1))
        diag = diag + (orbital(1, 1) * deep(4) + orbital(1, -1) * deep(5))
        diag = diag + (orbital(1, 0, 1) * flat(5) + orbital(1, 0, -1) * flat(6))
        back = orbital(0, -1) * deep(4, -1) + orbital(0, 1) * deep(5, 1)
        back = back + (orbital(0, 0, -1) * flat(5, -1) + orbital(0, 0, 1) * flat(6, 1))
        back = inner * (mid * flat(3)) + 2.0 * back
        rest[0, i, t] = centre[t] * (mid * flat(0)) + inner * near + (2.0 * diag + far)
        rest[1, i, t] = back
        rest[2, i, t] = mid * flat(4)

    def whole(slot, dst, fresh):
        for c in range(CHUNKS):
            widen(slot, dst, c)
        pad_start(dst)
        pad_end(dst)
        gather(slot, dst, fresh, 0, tiles)

    def edges_in(slot):
        edge_arrived(slot)

        @pl.when(slot == 2)
        def _():
            each_side(lambda side: edge_on(side).start())
            pl.when(is_b)(lambda: each_side(lambda side: edge_relay(side).start()))

    def chunk_in(slot, c):
        arrived(slot, c)

        @pl.when(slot == 2)
        def _():
            send_on(c).start()
            pl.when(is_b)(lambda: relay(c).start())

    edge_arrived(mine)
    weigh(mine, True)
    whole(mine, own, True)

    def total(t, i):
        return rest[0, i, t] + pltpu.roll(rest[1, i, t], 1, 1) + pltpu.roll(rest[2, i, t], 2, 1)

    def pair_of(n):
        return lax.rem(n + PAD + half, half)

    def turn(n):
        k = pair_of(n)
        for i in range(orbs):
            for h in range(2):
                rest[0, i, 2 * k + h] = total(2 * k + h, i)

    def store(n):
        k = pair_of(n)
        for i in range(orbs):
            a, b = shuffle(rest[0, i, 2 * k], rest[0, i, 2 * k + 1])
            out_ref[i, :, lane_tile(k)] = a
            out_ref[i, :, lane_tile(k + half)] = b

    def apply(n):
        store(n - 2)
        turn(n - 1)
        k = pair_of(n)
        for h in range(2):
            for i in range(orbs):
                finish(2 * k + h, i)

    order = (by_kind(3, 1, 2, 1), by_kind(2, 2, 1, 2), by_kind(1, 3, 3, 3))

    def visit(n, c):
        slot = order[n]
        dst = vis.at[n % 2]
        if c == 0:
            edges_in(slot)
            weigh(slot, False)
        chunk_in(slot, c)
        widen(slot, dst, c)
        if c == 0:
            pad_end(dst)
        first = 2 * bounds[c] - PAD if c else 1
        final = c == CHUNKS - 1
        gather(slot, dst, False, first, (tiles if final else 2 * bounds[c + 1] - PAD) - first)
        if final:
            pad_start(dst)
            gather(slot, dst, False, 0, 1)

    def direct_sent():
        each_side(lambda side: edge_copy(side, mine, 0).wait_send())
        each_side(lambda side: edge_copy(side, 2, 2).wait_send())
        each_side(lambda side: edge_on(side).wait_send())
        pl.when(is_b)(lambda: each_side(lambda side: edge_relay(side).wait_send()))
        for c in range(CHUNKS):
            send_x(c).wait_send()

        @pl.when(jnp.logical_not(is_d))
        def _():
            each_side(lambda side: edge_copy(side, slot_y, reach_y).wait_send())
            for c in range(CHUNKS):
                send_y(c).wait_send()

    applied = 0
    for c in range(CHUNKS):
        visit(0, c)
    visit(1, 0)
    for c in range(CHUNKS):
        final = c == CHUNKS - 1
        if not final:
            visit(1, c + 1)
        else:
            direct_sent()
        visit(2, c)
        if final:
            for n, (which, dy) in enumerate(FLAT):
                if dy > 0:
                    for p in range(dy):
                        gram[n, PAD - 1 - p] = seam(gram[n, PAD + tiles - 1 - p], False)
                if dy < 0:
                    gram[n, PAD + tiles] = seam(gram[n, PAD], True)
            for n, (which, dx, dy) in enumerate(WIDE):
                if dy > 0:
                    wide[n, PAD - 1] = seam(wide[n, PAD + tiles - 1], False)
                if dy < 0:
                    wide[n, PAD + tiles] = seam(wide[n, PAD], True)
        done = half if final else max((2 * bounds[c + 1] - PAD - 1) // 2 - PAD, 0)
        if done > applied:
            loop(done - applied, apply, done - applied, applied)
        applied = done
    store(half - 2)
    turn(half - 1)
    store(half - 1)

    for c in range(CHUNKS):
        send_on(c).wait_send()

        pl.when(is_b)(lambda c=c: relay(c).wait_send())


def per_device(n_band, n_slab, orbitals, occupation):
    orbs, planes, cells = orbitals.shape
    tiles = cells // LANES
    ext = -(-(planes + 2 * WIDTH) // 8) * 8
    tall = planes + 2 * TOP + 8
    occ = occupation.reshape(1, orbs)
    f32, bf16 = jnp.float32, jnp.bfloat16
    rows, groups = GROUP * orbs * WIDTH, tiles // (2 * GROUP)
    padded = tiles + 2 * PAD
    return pl.pallas_call(
        functools.partial(kernel, n_band, n_slab),
        out_shape=pltpu.VMEM(orbitals.shape, f32),
        in_specs=[pl.BlockSpec(memory_space=pl.ANY)] * 2,
        out_specs=pl.BlockSpec(memory_space=pltpu.VMEM),
        scratch_shapes=[
            pltpu.VMEM((SENDS, orbs, 2, planes, cells // 2), bf16),
            pltpu.VMEM((2, groups + 1, rows, 2 * LANES), bf16),
            pltpu.VMEM((SENDS, 2, groups + 1, rows, 2 * LANES), bf16),
            pltpu.VMEM((orbs, 3, padded, tall, LANES), f32),
            pltpu.VMEM((2, orbs, 3, padded, tall, LANES), f32),
            pltpu.VMEM((len(FLAT), padded, planes, LANES), f32),
            pltpu.VMEM((len(WIDE), padded, ext, LANES), f32),
            pltpu.VMEM((tiles, planes, LANES), f32),
            pltpu.VMEM((2 * LANES, 6 * LANES), bf16),
            pltpu.VMEM((3, orbs, tiles, planes, LANES), f32),
            pltpu.VMEM(occ.shape, bf16),
            pltpu.VMEM((SENDS, orbs, 8, LANES), f32),
            pltpu.SemaphoreType.DMA((3,)),
            pltpu.SemaphoreType.DMA((SENDS, CHUNKS)),
            pltpu.SemaphoreType.DMA((SENDS, CHUNKS)),
            pltpu.SemaphoreType.DMA((SENDS + 2, 2)),
            pltpu.SemaphoreType.DMA((SENDS, 2)),
        ],
        compiler_params=pltpu.CompilerParams(collective_id=0, has_side_effects=True),
        name="exchange",
    )(orbitals, occ)


def solution(mesh):
    in_specs = (P("band", "slab", None), P("band"))
    out_specs = P("band", "slab", None)
    return jax.shard_map(
        functools.partial(per_device, mesh.shape["band"], mesh.shape["slab"]),
        mesh=mesh, in_specs=in_specs, out_specs=out_specs, check_vma=False,
    )
```
